32 devices in a mesh: high: 8 (over z, core), low: 4 (over y, x).
Axes of the slice: x: 2, y: 2, z: 4, core: 2. Of those that a mesh axis runs over, the one named last changes fastest.
Arguments:
- wave_parts: float32 [2, 128, 128, 128], P(None, ('high', 'low')), may hold values from -6 to 6
- level_table: float32 [128, 128, 128], P(('high', 'low')), may hold values from -2 to 2
- phase_angles: float32 [2, 128], replicated, may hold values from 0.3 to 1.2
- mix_angles: float32 [2, 4], replicated, may hold values from 0.3 to 1.2
Outputs:
- result_parts: float32 [2, 128, 128, 128], P(None, ('high', 'low'))
- marginal: float32 [16, 128, 128], P('low', 'high')
The draws below stay inside these ranges and needn't reach their ends.
All inputs are finite; a program needn't handle non-finite values.
Results may differ from the reference program's by a relative error of at most 0.0003.
Values sent between devices are 32-bit elements; how exact they have to be, the bound alone decides.
No kernel may reach another device: no remote copies, remote signals or barrier semaphores. Data moves between devices by JAX's collectives and lax.ppermute only.
A program may use at most 64 MiB of HBM per device.

```python
import jax
import jax.numpy as jnp
from jax import lax

BLOCKS_DEV = 4
ROWS = 128
LANES = 128
BLOCKS = 128
LAYERS = 2
N_HIGH = 8
N_LOW = 4


def block_scale(stream_key, extent, cuts, least, high):
    factor_of = 1.0
    for dim, blocks in cuts:
        heights = jax.random.uniform(jax.random.fold_in(jax.random.fold_in(stream_key, 6), dim), (blocks,), jnp.float32, least / len(cuts), high / len(cuts))
        factor_of = factor_of * jnp.repeat(jnp.exp(heights), extent[dim] // blocks).reshape((-1,) + (1,) * (len(extent) - 1 - dim))
    return factor_of


def normal_values(key, extent, deviation, most, split=(), kind=jnp.bfloat16):
    level = block_scale(key, extent, split, -0.22, 0.18) if split else 1.0
    values = jax.random.normal(key, extent, jnp.float32) * deviation * level
    return jnp.minimum(jnp.maximum(values, -most), most).astype(kind)


def setup_inputs(seed: int = 0) -> dict:
    streams_of = jax.random.split(jax.random.key(seed), 5)
    wave_parts = normal_values(streams_of[0], (2, BLOCKS, ROWS, LANES), 1.0, 6.0, ((1, 32),), jnp.float32)
    level_table = jnp.clip(jax.random.uniform(streams_of[1], (BLOCKS, ROWS, LANES), jnp.float32, -2.0, 2.0) * block_scale(streams_of[1], (BLOCKS, ROWS, LANES), ((0, 32),), -0.4, 0.0), -2.0, 2.0)
    phase_angles = jnp.clip(jax.random.uniform(streams_of[2], (LAYERS, LANES), jnp.float32, 0.3, 1.2), 0.3, 1.2)
    mix_angles = jnp.clip(jax.random.uniform(streams_of[3], (LAYERS, 4), jnp.float32, 0.3, 1.2), 0.3, 1.2)
    return dict(wave_parts=wave_parts, level_table=level_table, phase_angles=phase_angles, mix_angles=mix_angles)


def count_bits(values, count):
    places = jnp.arange(count.bit_length() - 1, dtype=jnp.int32)
    return jnp.sum((values[..., None] >> places) & 1, axis=-1)


def real_turn_table(count, angle):
    rank = jnp.arange(count, dtype=jnp.int32)
    apart = count_bits(rank[:, None] ^ rank[None, :], count)
    minus = count_bits(rank[:, None] & (rank[:, None] ^ rank[None, :]), count)
    bits = count.bit_length() - 1
    size = jnp.cos(angle) ** (bits - apart).astype(jnp.float32) * jnp.sin(angle) ** apart.astype(jnp.float32)
    return size * jnp.where(minus % 2 == 1, -1.0, 1.0).astype(jnp.float32)


def apply_along(values, dim, angle):
    real_part = real_turn_table(values.shape[dim], angle)
    def times(table):
        moved = jnp.tensordot(values, table, axes=([dim], [0]), precision=lax.Precision.HIGHEST)
        return jnp.moveaxis(moved, -1, dim)
    return times(real_part)


def phase_step(values, levels, angle):
    turn = angle * levels
    return jnp.stack([values[0] * jnp.cos(turn) + values[1] * jnp.sin(turn), values[1] * jnp.cos(turn) - values[0] * jnp.sin(turn)])


def reference(wave_parts, level_table, phase_angles, mix_angles):
    values = wave_parts
    for layer in range(LAYERS):
        values = phase_step(values, level_table, phase_angles[layer])
        values = apply_along(values, 3, mix_angles[layer, 0])
        values = apply_along(values, 2, mix_angles[layer, 1])
        parts = values.reshape(2, N_HIGH, N_LOW, BLOCKS_DEV, ROWS, LANES)
        parts = apply_along(parts, 1, mix_angles[layer, 2])
        parts = apply_along(parts, 2, mix_angles[layer, 3])
        parts = apply_along(parts, 3, mix_angles[layer, 2])
        values = parts.reshape(values.shape)
    chance = values[0] * values[0] + values[1] * values[1]
    marginal = jnp.mean(chance.reshape(N_HIGH, -1, ROWS, LANES), axis=0)
    return values, marginal
```

```python
import functools

import jax
import jax.numpy as jnp
from jax import lax
from jax.experimental import pallas as pl
from jax.experimental.pallas import tpu as pltpu
from jax.sharding import PartitionSpec as P

AXES = ("high", "low")

SIN_TERMS = (1.0, -1.66666652e-01, 8.33326050e-03, -1.98281822e-04, 2.65947294e-06)
COS_TERMS = (9.99999995e-01, -4.99999845e-01, 4.16658692e-02, -1.38745501e-03, 2.37459074e-05)


def horner(terms, z):
    total = terms[-1]
    for term in terms[-2::-1]:
        total = total * z + term
    return total


def cos_sin(turn):
    half = turn * 0.5
    z = half * half
    s = half * horner(SIN_TERMS, z)
    c = horner(COS_TERMS, z)
    return 1.0 - 2.0 * s * s, 2.0 * s * c


def bits_of(count):
    return count.bit_length() - 1


def angle_row(angles, layer, group, lanes):
    return cos_sin(jnp.full((1, lanes), angles[layer, group], jnp.float32))


def turn_matrix(count, c, s, flip):
    row = lax.broadcasted_iota(jnp.int32, (count, count), 0)
    column = lax.broadcasted_iota(jnp.int32, (count, count), 1)
    apart = row ^ column
    up, down = (-s, s) if flip else (s, -s)
    total = None
    for bit in range(bits_of(count)):
        mask = 1 << bit
        side = jnp.where((column & mask) != 0, up, down)
        factor = jnp.where((apart & mask) != 0, side, c)
        total = factor if total is None else total * factor
    return total


def split(x):
    top = x.astype(jnp.bfloat16)
    return top, (x - top.astype(jnp.float32)).astype(jnp.bfloat16)


def butterflies(values, tangents):
    for bit, tangent in enumerate(tangents):
        new = list(values)
        for i in range(len(values)):
            j = i | (1 << bit)
            if i != j:
                new[i] = values[i] - tangent * values[j]
                new[j] = values[j] + tangent * values[i]
        values = new
    return values


def power(c, n):
    total = c
    for _ in range(n - 1):
        total = total * c
    return total


def mix_rows_lanes(parts, row_matrix, lane_matrix):
    rt, rl = row_matrix
    left = jnp.concatenate([rt, rl, rt], axis=1)
    tops, lows = zip(*[split(x) for x in parts])
    top, low = jnp.concatenate(tops, axis=1), jnp.concatenate(lows, axis=1)
    right = jnp.concatenate([top, top, low], axis=0)
    mixed = jnp.dot(left, right, preferred_element_type=jnp.float32)
    lt, ll = lane_matrix
    weights = jnp.concatenate([lt, ll, lt], axis=0)
    lanes = lt.shape[0]
    outs = []
    for i in range(len(parts)):
        t, l = split(mixed[:, i * lanes : (i + 1) * lanes])
        outs.append(jnp.dot(jnp.concatenate([t, t, l], axis=1), weights, preferred_element_type=jnp.float32))
    return outs


def first_kernel(wave, levels, phases, angles, out, work):
    _, blocks, rows, lanes = wave.shape
    chunk = out.shape[2]
    per = rows // chunk
    c2, s2 = angle_row(angles, 0, 2, lanes)
    scale = power(c2, bits_of(blocks)) if blocks > 1 else jnp.ones_like(c2)
    tangent = s2 / c2
    for t in range(blocks):
        level = levels[t]
        c, s = cos_sin(phases[0:1, :] * level)
        c, s = c * scale, s * scale
        re, im = wave[0, t], wave[1, t]
        work[0, t] = re * c + im * s
        work[1, t] = im * c - re * s
        out[per * t : per * (t + 1), 2] = level.reshape(per, chunk, lanes)
    c1, s1 = angle_row(angles, 0, 1, lanes)
    row_matrix = split(turn_matrix(rows, c1, s1, True))
    c0, s0 = angle_row(angles, 0, 0, lanes)
    lane_matrix = split(turn_matrix(lanes, c0, s0, False))
    for p in range(2):
        mixed = butterflies([work[p, t] for t in range(blocks)], [tangent] * bits_of(blocks))
        for t in range(blocks):
            work[p, t] = mixed[t]
    for t in range(blocks):
        for p, y in enumerate(mix_rows_lanes([work[0, t], work[1, t]], row_matrix, lane_matrix)):
            out[per * t : per * (t + 1), p] = y.reshape(per, chunk, lanes)


def device_kernel(highs, lows, got, phases, angles, out, work):
    count, _, chunk, lanes = got.shape
    low_bits, high_bits = bits_of(lows), bits_of(highs)
    tangents, scale = [], None
    for layer in range(2):
        c2, s2 = angle_row(angles, layer, 2, lanes)
        c3, s3 = angle_row(angles, layer, 3, lanes)
        tangents.append([s3 / c3] * low_bits + [s2 / c2] * high_bits)
        for c in [c3] * low_bits + [c2] * high_bits:
            scale = c if scale is None else scale * c
    for first in range(0, chunk, 8):
        rows = slice(first, first + 8)
        for p in range(2):
            mixed = butterflies([got[d, p, rows, :] for d in range(count)], tangents[0])
            for d in range(count):
                work[p, d] = mixed[d]
        for d in range(count):
            c, s = cos_sin(phases[1:2, :] * got[d, 2, rows, :])
            c, s = c * scale, s * scale
            re, im = work[0, d], work[1, d]
            work[0, d] = re * c + im * s
            work[1, d] = im * c - re * s
        for p in range(2):
            mixed = butterflies([work[p, d] for d in range(count)], tangents[1])
            for d in range(count):
                out[d, p, rows, :] = mixed[d]


def last_kernel(got, angles, out, keep, send, work, chance):
    _, blocks, rows, lanes = out.shape
    chunk = got.shape[2]
    per = rows // chunk
    pairs, _, part = keep.shape[0], keep.shape[1], keep.shape[2]
    c2, s2 = angle_row(angles, 1, 2, lanes)
    tangent = s2 / c2
    c1, s1 = angle_row(angles, 1, 1, lanes)
    row_matrix = split(turn_matrix(rows, c1, s1, True))
    c0, s0 = angle_row(angles, 1, 0, lanes)
    matrix = turn_matrix(lanes, c0, s0, False)
    if blocks > 1:
        matrix = matrix * power(c2, bits_of(blocks))
    lane_matrix = split(matrix)
    for p in range(2):
        loaded = [got[per * t : per * (t + 1), p].reshape(rows, lanes) for t in range(blocks)]
        mixed = butterflies(loaded, [tangent] * bits_of(blocks))
        for t in range(blocks):
            work[p, t] = mixed[t]
    for t in range(blocks):
        re, im = mix_rows_lanes([work[0, t], work[1, t]], row_matrix, lane_matrix)
        out[0, t] = re
        out[1, t] = im
        sizes = (re * re + im * im).reshape(pairs, 2, part, lanes)
        for side in range(2):
            chance[side, :, t] = sizes[:, side]
    side = lax.rem(lax.axis_index("high"), 2)
    keep[...] = chance[side]
    send[...] = chance[1 - side]


def pair_kernel(keep, got, own, *rest):
    sends, work = rest[:-1], rest[-1]
    work[...] = keep[...] + got[...]
    place = lax.div(lax.axis_index("high"), 2)
    own[...] = work[place]
    for k, send in enumerate(sends):
        send[...] = work[place ^ (k + 1)]


def sum_kernel(scale, *refs):
    total = refs[0][...]
    for ref in refs[1:-1]:
        total = total + ref[...]
    refs[-1][...] = total * scale


VMEM = pl.BlockSpec(memory_space=pltpu.VMEM)
SMEM = pl.BlockSpec(memory_space=pltpu.SMEM)


def call(kernel, name, out_shape, in_specs, scratch, args):
    many = isinstance(out_shape, (list, tuple))
    return pl.pallas_call(
        kernel,
        name=name,
        out_shape=out_shape,
        in_specs=in_specs,
        out_specs=[VMEM] * len(out_shape) if many else VMEM,
        scratch_shapes=scratch,
        compiler_params=pltpu.CompilerParams(vmem_limit_bytes=32 << 20),
    )(*args)


def spread(values):
    return lax.all_to_all(values, AXES, split_axis=0, concat_axis=0, tiled=True)


def shape_of(*extent):
    return jax.ShapeDtypeStruct(extent, jnp.float32)


def with_kernels(wave, levels, phases, angles):
    highs, lows = lax.axis_size("high"), lax.axis_size("low")
    _, blocks, rows, lanes = wave.shape
    count = highs * lows
    chunk = blocks * rows // count
    part = rows // highs
    pairs = highs // 2
    f32 = jnp.float32
    sent = call(first_kernel, "first", shape_of(count, 3, chunk, lanes), [VMEM, VMEM, VMEM, SMEM], [pltpu.VMEM(wave.shape, f32)], (wave, levels, phases, angles))
    mixed = call(
        functools.partial(device_kernel, highs, lows),
        "device",
        shape_of(count, 2, chunk, lanes),
        [VMEM, VMEM, SMEM],
        [pltpu.VMEM((2, count, 8, lanes), f32)],
        (spread(sent), phases, angles),
    )
    piece = shape_of(pairs, blocks, part, lanes)
    values, keep, send = call(
        last_kernel,
        "last",
        [shape_of(*wave.shape), piece, piece],
        [VMEM, SMEM],
        [pltpu.VMEM(wave.shape, f32), pltpu.VMEM((2, pairs, blocks, part, lanes), f32)],
        (spread(mixed), angles),
    )
    got = lax.ppermute(send, "high", [(i, i ^ 1) for i in range(highs)])
    own = shape_of(blocks, part, lanes)
    own, *sends = call(pair_kernel, "pair", [own] * pairs, [VMEM, VMEM], [pltpu.VMEM(piece.shape, f32)], (keep, got))
    others = [lax.ppermute(x, "high", [(i, i ^ (2 * (k + 1))) for i in range(highs)]) for k, x in enumerate(sends)]
    marginal = call(functools.partial(sum_kernel, 1.0 / highs), "sum", shape_of(blocks, part, lanes), [VMEM] * pairs, [], (own, *others))
    return values, marginal


def apply_along(values, dim, angle):
    count = values.shape[dim]
    table = turn_matrix(count, jnp.cos(angle), jnp.sin(angle), False) if count > 1 else jnp.ones((1, 1), jnp.float32)
    moved = jnp.tensordot(values, table, axes=([dim], [0]), precision=lax.Precision.HIGHEST)
    return jnp.moveaxis(moved, -1, dim)


def phase_step(re, im, levels, angle):
    c, s = cos_sin(angle * levels)
    return re * c + im * s, im * c - re * s


def with_arrays(wave, levels, phases, angles):
    highs, lows = lax.axis_size("high"), lax.axis_size("low")
    _, blocks, rows, lanes = wave.shape
    count = highs * lows
    chunk = blocks * rows // count

    def local(values, layer):
        values = apply_along(values, 3, angles[layer, 0])
        values = apply_along(values, 2, angles[layer, 1])
        return apply_along(values, 1, angles[layer, 2])

    def devices(values, layer):
        values = values.reshape(highs, lows, 2, chunk, lanes)
        values = apply_along(values, 0, angles[layer, 2])
        return apply_along(values, 1, angles[layer, 3]).reshape(count, 2, chunk, lanes)

    values = local(jnp.stack(phase_step(wave[0], wave[1], levels, phases[0])), 0)
    values = jnp.concatenate([values, levels[None]]).reshape(3, count, chunk, lanes).swapaxes(0, 1)
    values = spread(values)
    table = values[:, 2]
    values = devices(values[:, :2], 0)
    values = jnp.stack(phase_step(values[:, 0], values[:, 1], table, phases[1]), axis=1)
    values = spread(devices(values, 1)).swapaxes(0, 1).reshape(wave.shape)
    values = local(values, 1)
    chance = values[0] * values[0] + values[1] * values[1]
    return values, lax.psum_scatter(chance, "high", scatter_dimension=1, tiled=True) / highs


def on_device(wave, levels, phases, angles):
    highs, lows = lax.axis_size("high"), lax.axis_size("low")
    _, blocks, rows, _ = wave.shape
    whole_tiles = blocks * rows % (8 * highs * lows) == 0 and rows % (8 * highs) == 0
    within = rows % max(blocks * rows // (highs * lows), 1) == 0
    if whole_tiles and within and highs % 2 == 0:
        return with_kernels(wave, levels, phases, angles)
    return with_arrays(wave, levels, phases, angles)


def solution(mesh):
    in_specs = (P(None, AXES, None, None), P(AXES, None, None), P(), P())
    out_specs = (P(None, AXES, None, None), P("low", "high", None))
    return jax.shard_map(on_device, mesh=mesh, in_specs=in_specs, out_specs=out_specs, check_vma=False)
```

```python
import functools

import jax
import jax.numpy as jnp
from jax import lax
from jax.experimental import pallas as pl
from jax.experimental.pallas import tpu as pltpu
from jax.sharding import PartitionSpec as P

AXES = ("high", "low")

SIN_TERMS = (1.0, -1.66666652e-01, 8.33326050e-03, -1.98281822e-04, 2.65947294e-06)
COS_TERMS = (9.99999995e-01, -4.99999845e-01, 4.16658692e-02, -1.38745501e-03, 2.37459074e-05)


def horner(terms, z):
    total = terms[-1]
    for term in terms[-2::-1]:
        total = total * z + term
    return total


def cos_sin(turn):
    half = turn * 0.5
    z = half * half
    s = half * horner(SIN_TERMS, z)
    c = horner(COS_TERMS, z)
    return 1.0 - 2.0 * s * s, 2.0 * s * c


def bits_of(count):
    return count.bit_length() - 1


def angle_row(angles, layer, group, lanes):
    return cos_sin(jnp.full((1, lanes), angles[layer, group], jnp.float32))


def turn_matrix(count, c, s, flip):
    row = lax.broadcasted_iota(jnp.int32, (count, count), 0)
    column = lax.broadcasted_iota(jnp.int32, (count, count), 1)
    apart = row ^ column
    up, down = (-s, s) if flip else (s, -s)
    total = None
    for bit in range(bits_of(count)):
        mask = 1 << bit
        side = jnp.where((column & mask) != 0, up, down)
        factor = jnp.where((apart & mask) != 0, side, c)
        total = factor if total is None else total * factor
    return total


def split(x):
    top = x.astype(jnp.bfloat16)
    return top, (x - top.astype(jnp.float32)).astype(jnp.bfloat16)


def butterflies(values, tangents):
    for bit, tangent in enumerate(tangents):
        new = list(values)
        for i in range(len(values)):
            j = i | (1 << bit)
            if i != j:
                new[i] = values[i] - tangent * values[j]
                new[j] = values[j] + tangent * values[i]
        values = new
    return values


def power(c, n):
    total = c
    for _ in range(n - 1):
        total = total * c
    return total


def mix_rows_lanes(parts, row_matrix, lane_matrix):
    rt, rl = row_matrix
    left = jnp.concatenate([rt, rl, rt], axis=1)
    tops, lows = zip(*[split(x) for x in parts])
    top, low = jnp.concatenate(tops, axis=1), jnp.concatenate(lows, axis=1)
    right = jnp.concatenate([top, top, low], axis=0)
    mixed = jnp.dot(left, right, preferred_element_type=jnp.float32)
    lt, ll = lane_matrix
    weights = jnp.concatenate([lt, ll, lt], axis=0)
    lanes = lt.shape[0]
    outs = []
    for i in range(len(parts)):
        t, l = split(mixed[:, i * lanes : (i + 1) * lanes])
        outs.append(jnp.dot(jnp.concatenate([t, t, l], axis=1), weights, preferred_element_type=jnp.float32))
    return outs


def first_kernel(wave_there, levels_there, phases_there, angles_there, out, wave, levels, phases, angles, work, small, large):
    _, blocks, rows, lanes = wave.shape
    chunk = out.shape[2]
    per = rows // chunk
    pltpu.make_async_copy(angles_there, angles, small.at[0]).start()
    pltpu.make_async_copy(phases_there, phases, small.at[1]).start()
    copies = []
    for t in range(blocks):
        level = pltpu.make_async_copy(levels_there.at[t], levels.at[t], large.at[0, t])
        state = pltpu.make_async_copy(wave_there.at[:, t], wave.at[:, t], large.at[1, t])
        level.start()
        state.start()
        copies.append((level, state))
    pltpu.make_async_copy(angles_there, angles, small.at[0]).wait()
    c2, s2 = angle_row(angles, 0, 2, lanes)
    scale = power(c2, bits_of(blocks)) if blocks > 1 else jnp.ones_like(c2)
    tangent = s2 / c2
    c1, s1 = angle_row(angles, 0, 1, lanes)
    row_matrix = split(turn_matrix(rows, c1, s1, True))
    c0, s0 = angle_row(angles, 0, 0, lanes)
    lane_matrix = split(turn_matrix(lanes, c0, s0, False))
    pltpu.make_async_copy(phases_there, phases, small.at[1]).wait()
    for t in range(blocks):
        for copy in copies[t]:
            copy.wait()
        level = levels[t]
        c, s = cos_sin(phases[0:1, :] * level)
        c, s = c * scale, s * scale
        re, im = wave[0, t], wave[1, t]
        work[0, t] = re * c + im * s
        work[1, t] = im * c - re * s
        out[per * t : per * (t + 1), 2] = level.reshape(per, chunk, lanes)
    for p in range(2):
        mixed = butterflies([work[p, t] for t in range(blocks)], [tangent] * bits_of(blocks))
        for t in range(blocks):
            work[p, t] = mixed[t]
    for t in range(blocks):
        for p, y in enumerate(mix_rows_lanes([work[0, t], work[1, t]], row_matrix, lane_matrix)):
            out[per * t : per * (t + 1), p] = y.reshape(per, chunk, lanes)


def device_kernel(highs, lows, got, phases, angles, out, work):
    count, _, chunk, lanes = got.shape
    low_bits, high_bits = bits_of(lows), bits_of(highs)
    tangents, scale = [], None
    for layer in range(2):
        c2, s2 = angle_row(angles, layer, 2, lanes)
        c3, s3 = angle_row(angles, layer, 3, lanes)
        tangents.append([s3 / c3] * low_bits + [s2 / c2] * high_bits)
        for c in [c3] * low_bits + [c2] * high_bits:
            scale = c if scale is None else scale * c
    for first in range(0, chunk, 8):
        rows = slice(first, first + 8)
        for p in range(2):
            mixed = butterflies([got[d, p, rows, :] for d in range(count)], tangents[0])
            for d in range(count):
                work[p, d] = mixed[d]
        for d in range(count):
            c, s = cos_sin(phases[1:2, :] * got[d, 2, rows, :])
            c, s = c * scale, s * scale
            re, im = work[0, d], work[1, d]
            work[0, d] = re * c + im * s
            work[1, d] = im * c - re * s
        for p in range(2):
            mixed = butterflies([work[p, d] for d in range(count)], tangents[1])
            for d in range(count):
                out[d, p, rows, :] = mixed[d]


def last_kernel(got, angles, out_there, keep, send, work, out, chance, sems):
    _, blocks, rows, lanes = out.shape
    chunk = got.shape[2]
    per = rows // chunk
    pairs, _, part = keep.shape[0], keep.shape[1], keep.shape[2]
    c2, s2 = angle_row(angles, 1, 2, lanes)
    tangent = s2 / c2
    c1, s1 = angle_row(angles, 1, 1, lanes)
    row_matrix = split(turn_matrix(rows, c1, s1, True))
    c0, s0 = angle_row(angles, 1, 0, lanes)
    matrix = turn_matrix(lanes, c0, s0, False)
    if blocks > 1:
        matrix = matrix * power(c2, bits_of(blocks))
    lane_matrix = split(matrix)
    for p in range(2):
        loaded = [got[per * t : per * (t + 1), p].reshape(rows, lanes) for t in range(blocks)]
        mixed = butterflies(loaded, [tangent] * bits_of(blocks))
        for t in range(blocks):
            work[p, t] = mixed[t]
    for t in range(blocks):
        re, im = mix_rows_lanes([work[0, t], work[1, t]], row_matrix, lane_matrix)
        out[0, t] = re
        out[1, t] = im
        pltpu.make_async_copy(out.at[:, t], out_there.at[:, t], sems.at[t]).start()
        sizes = (re * re + im * im).reshape(pairs, 2, part, lanes)
        for side in range(2):
            chance[side, :, t] = sizes[:, side]
    side = lax.rem(lax.axis_index("high"), 2)
    keep[...] = chance[side]
    send[...] = chance[1 - side]
    for t in range(blocks):
        pltpu.make_async_copy(out.at[:, t], out_there.at[:, t], sems.at[t]).wait()


def pair_kernel(keep, got, own, *rest):
    sends, work = rest[:-1], rest[-1]
    work[...] = keep[...] + got[...]
    place = lax.div(lax.axis_index("high"), 2)
    own[...] = work[place]
    for k, send in enumerate(sends):
        send[...] = work[place ^ (k + 1)]


def sum_kernel(scale, *refs):
    total = refs[0][...]
    for ref in refs[1:-1]:
        total = total + ref[...]
    refs[-1][...] = total * scale


VMEM = pl.BlockSpec(memory_space=pltpu.VMEM)
SMEM = pl.BlockSpec(memory_space=pltpu.SMEM)
HBM = pl.BlockSpec(memory_space=pltpu.HBM)


def call(kernel, name, out_shape, in_specs, scratch, args, out_specs=None):
    many = isinstance(out_shape, (list, tuple))
    if out_specs is None:
        out_specs = [VMEM] * len(out_shape) if many else VMEM
    return pl.pallas_call(
        kernel,
        name=name,
        out_shape=out_shape,
        in_specs=in_specs,
        out_specs=out_specs,
        scratch_shapes=scratch,
        compiler_params=pltpu.CompilerParams(vmem_limit_bytes=32 << 20),
    )(*args)


def spread(values):
    return lax.all_to_all(values, AXES, split_axis=0, concat_axis=0, tiled=True)


def shape_of(*extent):
    return jax.ShapeDtypeStruct(extent, jnp.float32)


def with_kernels(wave, levels, phases, angles):
    highs, lows = lax.axis_size("high"), lax.axis_size("low")
    _, blocks, rows, lanes = wave.shape
    count = highs * lows
    chunk = blocks * rows // count
    part = rows // highs
    pairs = highs // 2
    f32 = jnp.float32
    sent = call(
        first_kernel,
        "first",
        shape_of(count, 3, chunk, lanes),
        [HBM] * 4,
        [
            pltpu.VMEM(wave.shape, f32),
            pltpu.VMEM(levels.shape, f32),
            pltpu.VMEM(phases.shape, f32),
            pltpu.SMEM(angles.shape, f32),
            pltpu.VMEM(wave.shape, f32),
            pltpu.SemaphoreType.DMA((2,)),
            pltpu.SemaphoreType.DMA((2, blocks)),
        ],
        tuple(pltpu.with_memory_space_constraint(x, pltpu.HBM) for x in (wave, levels, phases, angles)),
    )
    mixed = call(
        functools.partial(device_kernel, highs, lows),
        "device",
        shape_of(count, 2, chunk, lanes),
        [VMEM, VMEM, SMEM],
        [pltpu.VMEM((2, count, 8, lanes), f32)],
        (spread(sent), phases, angles),
    )
    piece = shape_of(pairs, blocks, part, lanes)
    values, keep, send = call(
        last_kernel,
        "last",
        [shape_of(*wave.shape), piece, piece],
        [VMEM, SMEM],
        [
            pltpu.VMEM(wave.shape, f32),
            pltpu.VMEM(wave.shape, f32),
            pltpu.VMEM((2, pairs, blocks, part, lanes), f32),
            pltpu.SemaphoreType.DMA((blocks,)),
        ],
        (spread(mixed), angles),
        [HBM, VMEM, VMEM],
    )
    got = lax.ppermute(send, "high", [(i, i ^ 1) for i in range(highs)])
    own = shape_of(blocks, part, lanes)
    own, *sends = call(pair_kernel, "pair", [own] * pairs, [VMEM, VMEM], [pltpu.VMEM(piece.shape, f32)], (keep, got))
    others = [lax.ppermute(x, "high", [(i, i ^ (2 * (k + 1))) for i in range(highs)]) for k, x in enumerate(sends)]
    marginal = call(functools.partial(sum_kernel, 1.0 / highs), "sum", shape_of(blocks, part, lanes), [VMEM] * pairs, [], (own, *others))
    return values, marginal


def apply_along(values, dim, angle):
    count = values.shape[dim]
    table = turn_matrix(count, jnp.cos(angle), jnp.sin(angle), False) if count > 1 else jnp.ones((1, 1), jnp.float32)
    moved = jnp.tensordot(values, table, axes=([dim], [0]), precision=lax.Precision.HIGHEST)
    return jnp.moveaxis(moved, -1, dim)


def phase_step(re, im, levels, angle):
    c, s = cos_sin(angle * levels)
    return re * c + im * s, im * c - re * s


def with_arrays(wave, levels, phases, angles):
    highs, lows = lax.axis_size("high"), lax.axis_size("low")
    _, blocks, rows, lanes = wave.shape
    count = highs * lows
    chunk = blocks * rows // count

    def local(values, layer):
        values = apply_along(values, 3, angles[layer, 0])
        values = apply_along(values, 2, angles[layer, 1])
        return apply_along(values, 1, angles[layer, 2])

    def devices(values, layer):
        values = values.reshape(highs, lows, 2, chunk, lanes)
        values = apply_along(values, 0, angles[layer, 2])
        return apply_along(values, 1, angles[layer, 3]).reshape(count, 2, chunk, lanes)

    values = local(jnp.stack(phase_step(wave[0], wave[1], levels, phases[0])), 0)
    values = jnp.concatenate([values, levels[None]]).reshape(3, count, chunk, lanes).swapaxes(0, 1)
    values = spread(values)
    table = values[:, 2]
    values = devices(values[:, :2], 0)
    values = jnp.stack(phase_step(values[:, 0], values[:, 1], table, phases[1]), axis=1)
    values = spread(devices(values, 1)).swapaxes(0, 1).reshape(wave.shape)
    values = local(values, 1)
    chance = values[0] * values[0] + values[1] * values[1]
    return values, lax.psum_scatter(chance, "high", scatter_dimension=1, tiled=True) / highs


def on_device(wave, levels, phases, angles):
    highs, lows = lax.axis_size("high"), lax.axis_size("low")
    _, blocks, rows, _ = wave.shape
    whole_tiles = blocks * rows % (8 * highs * lows) == 0 and rows % (8 * highs) == 0
    within = rows % max(blocks * rows // (highs * lows), 1) == 0
    if whole_tiles and within and highs % 2 == 0:
        return with_kernels(wave, levels, phases, angles)
    return with_arrays(wave, levels, phases, angles)


def solution(mesh):
    in_specs = (P(None, AXES, None, None), P(AXES, None, None), P(), P())
    out_specs = (P(None, AXES, None, None), P("low", "high", None))
    return jax.shard_map(on_device, mesh=mesh, in_specs=in_specs, out_specs=out_specs, check_vma=False)
```

```python
import functools

import jax
import jax.numpy as jnp
from jax import lax
from jax.experimental import pallas as pl
from jax.experimental.pallas import tpu as pltpu
from jax.sharding import PartitionSpec as P

AXES = ("high", "low")

SIN_TERMS = (1.0, -1.66666652e-01, 8.33326050e-03, -1.98281822e-04, 2.65947294e-06)
COS_TERMS = (9.99999995e-01, -4.99999845e-01, 4.16658692e-02, -1.38745501e-03, 2.37459074e-05)


def horner(terms, z):
    total = terms[-1]
    for term in terms[-2::-1]:
        total = total * z + term
    return total


def cos_sin(turn):
    half = turn * 0.5
    z = half * half
    s = half * horner(SIN_TERMS, z)
    c = horner(COS_TERMS, z)
    return 1.0 - 2.0 * s * s, 2.0 * s * c


def bits_of(count):
    return count.bit_length() - 1


def angle_row(angles, layer, group, lanes):
    return cos_sin(jnp.full((1, lanes), angles[layer, group], jnp.float32))


def turn_matrix(count, c, s, flip):
    up, down = (-s, s) if flip else (s, -s)
    height = min(count, 8)
    row = lax.broadcasted_iota(jnp.int32, (height, count), 0)
    column = lax.broadcasted_iota(jnp.int32, (height, count), 1)

    def sides(bit):
        there = (column & (1 << bit)) != 0
        return jnp.where(there, up, c), jnp.where(there, c, down)

    tile = jnp.ones((height, count), jnp.float32)
    for bit in range(bits_of(height)):
        low, high = sides(bit)
        tile = tile * jnp.where((row & (1 << bit)) != 0, high, low)
    tiles = [tile]
    for bit in range(bits_of(height), bits_of(count)):
        low, high = sides(bit)
        tiles = [x * low for x in tiles] + [x * high for x in tiles]
    return jnp.concatenate(tiles, axis=0) if len(tiles) > 1 else tiles[0]


def split(x):
    top = x.astype(jnp.bfloat16)
    return top, (x - top.astype(jnp.float32)).astype(jnp.bfloat16)


def butterflies(values, tangents):
    for bit, tangent in enumerate(tangents):
        new = list(values)
        for i in range(len(values)):
            j = i | (1 << bit)
            if i != j:
                new[i] = values[i] - tangent * values[j]
                new[j] = values[j] + tangent * values[i]
        values = new
    return values


def power(c, n):
    total = c
    for _ in range(n - 1):
        total = total * c
    return total


def mix_rows_lanes(parts, row_matrix, lane_matrix):
    rt, rl = row_matrix
    left = jnp.concatenate([rt, rl, rt], axis=1)
    tops, lows = zip(*[split(x) for x in parts])
    top, low = jnp.concatenate(tops, axis=1), jnp.concatenate(lows, axis=1)
    right = jnp.concatenate([top, top, low], axis=0)
    mixed = jnp.dot(left, right, preferred_element_type=jnp.float32)
    lt, ll = lane_matrix
    weights = jnp.concatenate([lt, ll, lt], axis=0)
    lanes = lt.shape[0]
    outs = []
    for i in range(len(parts)):
        t, l = split(mixed[:, i * lanes : (i + 1) * lanes])
        outs.append(jnp.dot(jnp.concatenate([t, t, l], axis=1), weights, preferred_element_type=jnp.float32))
    return outs


def first_kernel(wave_there, levels_there, phases_there, angles_there, out, wave, levels, phases, angles, work, small, large):
    _, blocks, rows, lanes = wave.shape
    chunk = out.shape[2]
    per = rows // chunk

    def level_copy(t):
        return pltpu.make_async_copy(levels_there.at[t], levels.at[t], large.at[0, t])

    def state_copy(t):
        return pltpu.make_async_copy(wave_there.at[:, t], wave.at[:, t], large.at[1, t])

    pltpu.make_async_copy(angles_there, angles, small.at[0]).start()
    pltpu.make_async_copy(phases_there, phases, small.at[1]).start()
    for t in range(blocks):
        level_copy(t).start()
        state_copy(t).start()
    pltpu.make_async_copy(angles_there, angles, small.at[0]).wait()
    c2, s2 = angle_row(angles, 0, 2, lanes)
    scale = power(c2, bits_of(blocks)) if blocks > 1 else jnp.ones_like(c2)
    tangents = [s2 / c2] * bits_of(blocks)
    c1, s1 = angle_row(angles, 0, 1, lanes)
    row_matrix = split(turn_matrix(rows, c1, s1, True))
    c0, s0 = angle_row(angles, 0, 0, lanes)
    lane_matrix = split(turn_matrix(lanes, c0, s0, False))
    pltpu.make_async_copy(phases_there, phases, small.at[1]).wait()
    angle = phases[0:1, :]

    def block(t, carry):
        level_copy(t).wait()
        state_copy(t).wait()
        level = levels[t]
        c, s = cos_sin(angle * level)
        c, s = c * scale, s * scale
        re, im = wave[0, t], wave[1, t]
        for p, y in enumerate(mix_rows_lanes([re * c + im * s, im * c - re * s], row_matrix, lane_matrix)):
            work[p, t] = y
        out[pl.ds(per * t, per), 2] = level.reshape(per, chunk, lanes)
        return carry

    lax.fori_loop(0, blocks, block, 0)

    def piece(i, carry):
        p, k = i // per, i % per
        mixed = butterflies([work[p, t, pl.ds(pl.multiple_of(chunk * k, 8), chunk), :] for t in range(blocks)], tangents)
        for t in range(blocks):
            out[per * t + k, p] = mixed[t]
        return carry

    lax.fori_loop(0, 2 * per, piece, 0)


def device_kernel(highs, lows, got, phases, angles, out, work):
    count, _, chunk, lanes = got.shape
    low_bits, high_bits = bits_of(lows), bits_of(highs)
    tangents, scale = [], None
    for layer in range(2):
        c2, s2 = angle_row(angles, layer, 2, lanes)
        c3, s3 = angle_row(angles, layer, 3, lanes)
        tangents.append([s3 / c3] * low_bits + [s2 / c2] * high_bits)
        for c in [c3] * low_bits + [c2] * high_bits:
            scale = c if scale is None else scale * c
    angle = phases[1:2, :]

    def tile(i, carry):
        rows = pl.ds(pl.multiple_of(8 * i, 8), 8)

        def before(p, carry):
            mixed = butterflies([got[d, p, rows, :] for d in range(count)], tangents[0])
            for d in range(count):
                work[p, d] = mixed[d]
            return carry

        def turn(k, carry):
            for d in range(8):
                d = 8 * k + d
                c, s = cos_sin(angle * got[d, 2, rows, :])
                c, s = c * scale, s * scale
                re, im = work[0, d], work[1, d]
                work[0, d] = re * c + im * s
                work[1, d] = im * c - re * s
            return carry

        def after(p, carry):
            mixed = butterflies([work[p, d] for d in range(count)], tangents[1])
            for d in range(count):
                out[d, p, rows, :] = mixed[d]
            return carry

        lax.fori_loop(0, 2, before, 0)
        lax.fori_loop(0, count // 8, turn, 0)
        lax.fori_loop(0, 2, after, 0)
        return carry

    lax.fori_loop(0, chunk // 8, tile, 0)


def last_kernel(got, angles, out, keep, send, work, chance):
    _, blocks, rows, lanes = out.shape
    chunk = got.shape[2]
    per = rows // chunk
    pairs, _, part = keep.shape[0], keep.shape[1], keep.shape[2]
    c2, s2 = angle_row(angles, 1, 2, lanes)
    tangents = [s2 / c2] * bits_of(blocks)
    c1, s1 = angle_row(angles, 1, 1, lanes)
    row_matrix = split(turn_matrix(rows, c1, s1, True))
    c0, s0 = angle_row(angles, 1, 0, lanes)
    matrix = turn_matrix(lanes, c0, s0, False)
    if blocks > 1:
        matrix = matrix * power(c2, bits_of(blocks))
    lane_matrix = split(matrix)

    def piece(i, carry):
        p, k = i // per, i % per
        mixed = butterflies([got[per * t + k, p] for t in range(blocks)], tangents)
        for t in range(blocks):
            work[p, t, pl.ds(pl.multiple_of(chunk * k, 8), chunk), :] = mixed[t]
        return carry

    lax.fori_loop(0, 2 * per, piece, 0)

    def block(t, carry):
        re, im = mix_rows_lanes([work[0, t], work[1, t]], row_matrix, lane_matrix)
        out[0, t] = re
        out[1, t] = im
        sizes = (re * re + im * im).reshape(pairs, 2, part, lanes)
        for side in range(2):
            chance[side, :, t] = sizes[:, side]
        return carry

    lax.fori_loop(0, blocks, block, 0)
    side = lax.rem(lax.axis_index("high"), 2)
    keep[...] = chance[side]
    send[...] = chance[1 - side]


def pair_kernel(keep, got, own, *rest):
    sends, work = rest[:-1], rest[-1]
    work[...] = keep[...] + got[...]
    place = lax.div(lax.axis_index("high"), 2)
    own[...] = work[place]
    for k, send in enumerate(sends):
        send[...] = work[place ^ (k + 1)]


def sum_kernel(scale, *refs):
    total = refs[0][...]
    for ref in refs[1:-1]:
        total = total + ref[...]
    refs[-1][...] = total * scale


VMEM = pl.BlockSpec(memory_space=pltpu.VMEM)
SMEM = pl.BlockSpec(memory_space=pltpu.SMEM)
HBM = pl.BlockSpec(memory_space=pltpu.HBM)


def call(kernel, name, out_shape, in_specs, scratch, args, out_specs=None):
    many = isinstance(out_shape, (list, tuple))
    if out_specs is None:
        out_specs = [VMEM] * len(out_shape) if many else VMEM
    return pl.pallas_call(
        kernel,
        name=name,
        out_shape=out_shape,
        in_specs=in_specs,
        out_specs=out_specs,
        scratch_shapes=scratch,
        compiler_params=pltpu.CompilerParams(vmem_limit_bytes=32 << 20),
    )(*args)


def spread(values):
    return lax.all_to_all(values, AXES, split_axis=0, concat_axis=0, tiled=True)


def shape_of(*extent):
    return jax.ShapeDtypeStruct(extent, jnp.float32)


def with_kernels(wave, levels, phases, angles):
    highs, lows = lax.axis_size("high"), lax.axis_size("low")
    _, blocks, rows, lanes = wave.shape
    count = highs * lows
    chunk = blocks * rows // count
    part = rows // highs
    pairs = highs // 2
    f32 = jnp.float32
    sent = call(
        first_kernel,
        "first",
        shape_of(count, 3, chunk, lanes),
        [HBM] * 4,
        [
            pltpu.VMEM(wave.shape, f32),
            pltpu.VMEM(levels.shape, f32),
            pltpu.VMEM(phases.shape, f32),
            pltpu.SMEM(angles.shape, f32),
            pltpu.VMEM(wave.shape, f32),
            pltpu.SemaphoreType.DMA((2,)),
            pltpu.SemaphoreType.DMA((2, blocks)),
        ],
        tuple(pltpu.with_memory_space_constraint(x, pltpu.HBM) for x in (wave, levels, phases, angles)),
    )
    mixed = call(
        functools.partial(device_kernel, highs, lows),
        "device",
        shape_of(count, 2, chunk, lanes),
        [VMEM, VMEM, SMEM],
        [pltpu.VMEM((2, count, 8, lanes), f32)],
        (spread(sent), phases, angles),
    )
    piece = shape_of(pairs, blocks, part, lanes)
    values, keep, send = call(
        last_kernel,
        "last",
        [pltpu.VMEM(wave.shape, f32), piece, piece],
        [VMEM, SMEM],
        [pltpu.VMEM(wave.shape, f32), pltpu.VMEM((2, pairs, blocks, part, lanes), f32)],
        (spread(mixed), angles),
    )
    got = lax.ppermute(send, "high", [(i, i ^ 1) for i in range(highs)])
    own = shape_of(blocks, part, lanes)
    own, *sends = call(pair_kernel, "pair", [own] * pairs, [VMEM, VMEM], [pltpu.VMEM(piece.shape, f32)], (keep, got))
    others = [lax.ppermute(x, "high", [(i, i ^ (2 * (k + 1))) for i in range(highs)]) for k, x in enumerate(sends)]
    marginal = call(functools.partial(sum_kernel, 1.0 / highs), "sum", shape_of(blocks, part, lanes), [VMEM] * pairs, [], (own, *others))
    return values, marginal


def apply_along(values, dim, angle):
    count = values.shape[dim]
    table = turn_matrix(count, jnp.cos(angle), jnp.sin(angle), False) if count > 1 else jnp.ones((1, 1), jnp.float32)
    moved = jnp.tensordot(values, table, axes=([dim], [0]), precision=lax.Precision.HIGHEST)
    return jnp.moveaxis(moved, -1, dim)


def phase_step(re, im, levels, angle):
    c, s = cos_sin(angle * levels)
    return re * c + im * s, im * c - re * s


def with_arrays(wave, levels, phases, angles):
    highs, lows = lax.axis_size("high"), lax.axis_size("low")
    _, blocks, rows, lanes = wave.shape
    count = highs * lows
    chunk = blocks * rows // count

    def local(values, layer):
        values = apply_along(values, 3, angles[layer, 0])
        values = apply_along(values, 2, angles[layer, 1])
        return apply_along(values, 1, angles[layer, 2])

    def devices(values, layer):
        values = values.reshape(highs, lows, 2, chunk, lanes)
        values = apply_along(values, 0, angles[layer, 2])
        return apply_along(values, 1, angles[layer, 3]).reshape(count, 2, chunk, lanes)

    values = local(jnp.stack(phase_step(wave[0], wave[1], levels, phases[0])), 0)
    values = jnp.concatenate([values, levels[None]]).reshape(3, count, chunk, lanes).swapaxes(0, 1)
    values = spread(values)
    table = values[:, 2]
    values = devices(values[:, :2], 0)
    values = jnp.stack(phase_step(values[:, 0], values[:, 1], table, phases[1]), axis=1)
    values = spread(devices(values, 1)).swapaxes(0, 1).reshape(wave.shape)
    values = local(values, 1)
    chance = values[0] * values[0] + values[1] * values[1]
    return values, lax.psum_scatter(chance, "high", scatter_dimension=1, tiled=True) / highs


def on_device(wave, levels, phases, angles):
    highs, lows = lax.axis_size("high"), lax.axis_size("low")
    _, blocks, rows, _ = wave.shape
    whole_tiles = blocks * rows % (8 * highs * lows) == 0 and rows % (8 * highs) == 0
    within = rows % max(blocks * rows // (highs * lows), 1) == 0
    if whole_tiles and within and highs % 2 == 0:
        return with_kernels(wave, levels, phases, angles)
    return with_arrays(wave, levels, phases, angles)


def solution(mesh):
    in_specs = (P(None, AXES, None, None), P(AXES, None, None), P(), P())
    out_specs = (P(None, AXES, None, None), P("low", "high", None))
    return jax.shard_map(on_device, mesh=mesh, in_specs=in_specs, out_specs=out_specs, check_vma=False)
```

```python
import functools

import jax
import jax.numpy as jnp
from jax import lax
from jax.experimental import pallas as pl
from jax.experimental.pallas import tpu as pltpu
from jax.sharding import PartitionSpec as P

AXES = ("high", "low")

SIN_TERMS = (1.0, -1.66666652e-01, 8.33326050e-03, -1.98281822e-04, 2.65947294e-06)
COS_TERMS = (9.99999995e-01, -4.99999845e-01, 4.16658692e-02, -1.38745501e-03, 2.37459074e-05)


def horner(terms, z):
    total = terms[-1]
    for term in terms[-2::-1]:
        total = total * z + term
    return total


def cos_sin(turn):
    half = turn * 0.5
    z = half * half
    s = half * horner(SIN_TERMS, z)
    c = horner(COS_TERMS, z)
    return 1.0 - 2.0 * s * s, 2.0 * s * c


def bits_of(count):
    return count.bit_length() - 1


def angle_row(angles, layer, group, lanes):
    return cos_sin(jnp.full((1, lanes), angles[layer, group], jnp.float32))


def turn_matrix(count, c, s, flip):
    up, down = (-s, s) if flip else (s, -s)
    height = min(count, 8)
    row = lax.broadcasted_iota(jnp.int32, (height, count), 0)
    column = lax.broadcasted_iota(jnp.int32, (height, count), 1)

    def sides(bit):
        there = (column & (1 << bit)) != 0
        return jnp.where(there, up, c), jnp.where(there, c, down)

    tile = jnp.ones((height, count), jnp.float32)
    for bit in range(bits_of(height)):
        low, high = sides(bit)
        tile = tile * jnp.where((row & (1 << bit)) != 0, high, low)
    tiles = [tile]
    for bit in range(bits_of(height), bits_of(count)):
        low, high = sides(bit)
        tiles = [x * low for x in tiles] + [x * high for x in tiles]
    return jnp.concatenate(tiles, axis=0) if len(tiles) > 1 else tiles[0]


def split(x):
    top = x.astype(jnp.bfloat16)
    return top, (x - top.astype(jnp.float32)).astype(jnp.bfloat16)


def butterflies(values, tangents):
    for bit, tangent in enumerate(tangents):
        new = list(values)
        for i in range(len(values)):
            j = i | (1 << bit)
            if i != j:
                new[i] = values[i] - tangent * values[j]
                new[j] = values[j] + tangent * values[i]
        values = new
    return values


def power(c, n):
    total = c
    for _ in range(n - 1):
        total = total * c
    return total


def mix_rows(parts, matrix):
    high, low = matrix
    left = jnp.concatenate([high, low, high], axis=1)
    highs, lows = zip(*[split(x) for x in parts])
    high, low = jnp.concatenate(highs, axis=1), jnp.concatenate(lows, axis=1)
    return jnp.dot(left, jnp.concatenate([high, high, low], axis=0), preferred_element_type=jnp.float32)


def mix_lanes(x, matrix):
    high, low = matrix
    top, rest = split(x)
    left = jnp.concatenate([top, top, rest], axis=1)
    return jnp.dot(left, jnp.concatenate([high, low, high], axis=0), preferred_element_type=jnp.float32)


def first_kernel(wave_there, levels_there, phases_there, angles_there, out, wave, levels, phases, angles, work, small, large):
    _, blocks, rows, lanes = wave.shape
    chunk = out.shape[2]
    per = rows // chunk

    def level_copy(t):
        return pltpu.make_async_copy(levels_there.at[t], levels.at[t], large.at[0, t])

    def state_copy(t):
        return pltpu.make_async_copy(wave_there.at[:, t], wave.at[:, t], large.at[1, t])

    pltpu.make_async_copy(angles_there, angles, small.at[0]).start()
    pltpu.make_async_copy(phases_there, phases, small.at[1]).start()
    for t in range(blocks):
        level_copy(t).start()
        state_copy(t).start()
    pltpu.make_async_copy(angles_there, angles, small.at[0]).wait()
    c2, s2 = angle_row(angles, 0, 2, lanes)
    scale = power(c2, bits_of(blocks)) if blocks > 1 else jnp.ones_like(c2)
    tangents = [s2 / c2] * bits_of(blocks)
    c1, s1 = angle_row(angles, 0, 1, lanes)
    row_matrix = split(turn_matrix(rows, c1, s1, True))
    c0, s0 = angle_row(angles, 0, 0, lanes)
    lane_matrix = split(turn_matrix(lanes, c0, s0, False))
    pltpu.make_async_copy(phases_there, phases, small.at[1]).wait()
    angle = phases[0:1, :]

    for t in range(blocks):
        level_copy(t).wait()
        state_copy(t).wait()
        level = levels[t]
        c, s = cos_sin(angle * level)
        c, s = c * scale, s * scale
        re, im = wave[0, t], wave[1, t]
        both = mix_rows([re * c + im * s, im * c - re * s], row_matrix)
        for p in range(2):
            work[p, t] = both[:, lanes * p : lanes * (p + 1)]
        out[per * t : per * (t + 1), 2] = level.reshape(per, chunk, lanes)
    for p in range(2):
        for k in range(per):
            rows_k = slice(chunk * k, chunk * (k + 1))
            mixed = butterflies([work[p, t, rows_k, :] for t in range(blocks)], tangents)
            for t in range(blocks):
                work[p, t, rows_k, :] = mixed[t]
    for p in range(2):
        for t in range(blocks):
            out[per * t : per * (t + 1), p] = mix_lanes(work[p, t], lane_matrix).reshape(per, chunk, lanes)


def device_kernel(highs, lows, got, phases, angles, out, work):
    count, _, chunk, lanes = got.shape
    low_bits, high_bits = bits_of(lows), bits_of(highs)
    tangents, scale = [], None
    for layer in range(2):
        c2, s2 = angle_row(angles, layer, 2, lanes)
        c3, s3 = angle_row(angles, layer, 3, lanes)
        tangents.append([s3 / c3] * low_bits + [s2 / c2] * high_bits)
        for c in [c3] * low_bits + [c2] * high_bits:
            scale = c if scale is None else scale * c
    angle = phases[1:2, :]

    for first in range(0, chunk, 8):
        rows = slice(first, first + 8)
        for p in range(2):
            mixed = butterflies([got[d, p, rows, :] for d in range(count)], tangents[0])
            for d in range(count):
                work[p, d] = mixed[d]
        for d in range(count):
            c, s = cos_sin(angle * got[d, 2, rows, :])
            c, s = c * scale, s * scale
            re, im = work[0, d], work[1, d]
            work[0, d] = re * c + im * s
            work[1, d] = im * c - re * s
        for p in range(2):
            mixed = butterflies([work[p, d] for d in range(count)], tangents[1])
            for d in range(count):
                out[d, p, rows, :] = mixed[d]


def last_kernel(got, angles, out, keep, send, work, chance):
    _, blocks, rows, lanes = out.shape
    chunk = got.shape[2]
    per = rows // chunk
    pairs, _, part = keep.shape[0], keep.shape[1], keep.shape[2]
    c2, s2 = angle_row(angles, 1, 2, lanes)
    tangents = [s2 / c2] * bits_of(blocks)
    c1, s1 = angle_row(angles, 1, 1, lanes)
    row_matrix = split(turn_matrix(rows, c1, s1, True))
    c0, s0 = angle_row(angles, 1, 0, lanes)
    matrix = turn_matrix(lanes, c0, s0, False)
    if blocks > 1:
        matrix = matrix * power(c2, bits_of(blocks))
    lane_matrix = split(matrix)

    for t in range(blocks):
        both = mix_rows([got[per * t : per * (t + 1), p].reshape(rows, lanes) for p in range(2)], row_matrix)
        for p in range(2):
            work[p, t] = both[:, lanes * p : lanes * (p + 1)]
    for p in range(2):
        for k in range(per):
            rows_k = slice(chunk * k, chunk * (k + 1))
            mixed = butterflies([work[p, t, rows_k, :] for t in range(blocks)], tangents)
            for t in range(blocks):
                work[p, t, rows_k, :] = mixed[t]
    for t in range(blocks):
        re, im = mix_lanes(work[0, t], lane_matrix), mix_lanes(work[1, t], lane_matrix)
        out[0, t] = re
        out[1, t] = im
        sizes = (re * re + im * im).reshape(pairs, 2, part, lanes)
        for side in range(2):
            chance[side, :, t] = sizes[:, side]
    side = lax.rem(lax.axis_index("high"), 2)
    keep[...] = chance[side]
    send[...] = chance[1 - side]


def pair_kernel(keep, got, own, *rest):
    sends, work = rest[:-1], rest[-1]
    work[...] = keep[...] + got[...]
    place = lax.div(lax.axis_index("high"), 2)
    own[...] = work[place]
    for k, send in enumerate(sends):
        send[...] = work[place ^ (k + 1)]


def sum_kernel(scale, *refs):
    total = refs[0][...]
    for ref in refs[1:-1]:
        total = total + ref[...]
    refs[-1][...] = total * scale


VMEM = pl.BlockSpec(memory_space=pltpu.VMEM)
SMEM = pl.BlockSpec(memory_space=pltpu.SMEM)
HBM = pl.BlockSpec(memory_space=pltpu.HBM)


def call(kernel, name, out_shape, in_specs, scratch, args, out_specs=None):
    many = isinstance(out_shape, (list, tuple))
    if out_specs is None:
        out_specs = [VMEM] * len(out_shape) if many else VMEM
    return pl.pallas_call(
        kernel,
        name=name,
        out_shape=out_shape,
        in_specs=in_specs,
        out_specs=out_specs,
        scratch_shapes=scratch,
        compiler_params=pltpu.CompilerParams(vmem_limit_bytes=32 << 20),
    )(*args)


def spread(values):
    return lax.all_to_all(values, AXES, split_axis=0, concat_axis=0, tiled=True)


def shape_of(*extent):
    return jax.ShapeDtypeStruct(extent, jnp.float32)


def with_kernels(wave, levels, phases, angles):
    highs, lows = lax.axis_size("high"), lax.axis_size("low")
    _, blocks, rows, lanes = wave.shape
    count = highs * lows
    chunk = blocks * rows // count
    part = rows // highs
    pairs = highs // 2
    f32 = jnp.float32
    sent = call(
        first_kernel,
        "first",
        shape_of(count, 3, chunk, lanes),
        [HBM] * 4,
        [
            pltpu.VMEM(wave.shape, f32),
            pltpu.VMEM(levels.shape, f32),
            pltpu.VMEM(phases.shape, f32),
            pltpu.SMEM(angles.shape, f32),
            pltpu.VMEM(wave.shape, f32),
            pltpu.SemaphoreType.DMA((2,)),
            pltpu.SemaphoreType.DMA((2, blocks)),
        ],
        tuple(pltpu.with_memory_space_constraint(x, pltpu.HBM) for x in (wave, levels, phases, angles)),
    )
    mixed = call(
        functools.partial(device_kernel, highs, lows),
        "device",
        shape_of(count, 2, chunk, lanes),
        [VMEM, VMEM, SMEM],
        [pltpu.VMEM((2, count, 8, lanes), f32)],
        (spread(sent), phases, angles),
    )
    piece = shape_of(pairs, blocks, part, lanes)
    values, keep, send = call(
        last_kernel,
        "last",
        [pltpu.VMEM(wave.shape, f32), piece, piece],
        [VMEM, SMEM],
        [pltpu.VMEM(wave.shape, f32), pltpu.VMEM((2, pairs, blocks, part, lanes), f32)],
        (spread(mixed), angles),
    )
    got = lax.ppermute(send, "high", [(i, i ^ 1) for i in range(highs)])
    own = shape_of(blocks, part, lanes)
    own, *sends = call(pair_kernel, "pair", [own] * pairs, [VMEM, VMEM], [pltpu.VMEM(piece.shape, f32)], (keep, got))
    others = [lax.ppermute(x, "high", [(i, i ^ (2 * (k + 1))) for i in range(highs)]) for k, x in enumerate(sends)]
    marginal = call(functools.partial(sum_kernel, 1.0 / highs), "sum", shape_of(blocks, part, lanes), [VMEM] * pairs, [], (own, *others))
    return values, marginal


def apply_along(values, dim, angle):
    count = values.shape[dim]
    table = turn_matrix(count, jnp.cos(angle), jnp.sin(angle), False) if count > 1 else jnp.ones((1, 1), jnp.float32)
    moved = jnp.tensordot(values, table, axes=([dim], [0]), precision=lax.Precision.HIGHEST)
    return jnp.moveaxis(moved, -1, dim)


def phase_step(re, im, levels, angle):
    c, s = cos_sin(angle * levels)
    return re * c + im * s, im * c - re * s


def with_arrays(wave, levels, phases, angles):
    highs, lows = lax.axis_size("high"), lax.axis_size("low")
    _, blocks, rows, lanes = wave.shape
    count = highs * lows
    chunk = blocks * rows // count

    def local(values, layer):
        values = apply_along(values, 3, angles[layer, 0])
        values = apply_along(values, 2, angles[layer, 1])
        return apply_along(values, 1, angles[layer, 2])

    def devices(values, layer):
        values = values.reshape(highs, lows, 2, chunk, lanes)
        values = apply_along(values, 0, angles[layer, 2])
        return apply_along(values, 1, angles[layer, 3]).reshape(count, 2, chunk, lanes)

    values = local(jnp.stack(phase_step(wave[0], wave[1], levels, phases[0])), 0)
    values = jnp.concatenate([values, levels[None]]).reshape(3, count, chunk, lanes).swapaxes(0, 1)
    values = spread(values)
    table = values[:, 2]
    values = devices(values[:, :2], 0)
    values = jnp.stack(phase_step(values[:, 0], values[:, 1], table, phases[1]), axis=1)
    values = spread(devices(values, 1)).swapaxes(0, 1).reshape(wave.shape)
    values = local(values, 1)
    chance = values[0] * values[0] + values[1] * values[1]
    return values, lax.psum_scatter(chance, "high", scatter_dimension=1, tiled=True) / highs


def on_device(wave, levels, phases, angles):
    highs, lows = lax.axis_size("high"), lax.axis_size("low")
    _, blocks, rows, _ = wave.shape
    whole_tiles = blocks * rows % (8 * highs * lows) == 0 and rows % (8 * highs) == 0
    within = rows % max(blocks * rows // (highs * lows), 1) == 0
    if whole_tiles and within and highs % 2 == 0:
        return with_kernels(wave, levels, phases, angles)
    return with_arrays(wave, levels, phases, angles)


def solution(mesh):
    in_specs = (P(None, AXES, None, None), P(AXES, None, None), P(), P())
    out_specs = (P(None, AXES, None, None), P("low", "high", None))
    return jax.shard_map(on_device, mesh=mesh, in_specs=in_specs, out_specs=out_specs, check_vma=False)
```

```python
import functools

import jax
import jax.numpy as jnp
from jax import lax
from jax.experimental import pallas as pl
from jax.experimental.pallas import tpu as pltpu
from jax.sharding import PartitionSpec as P

AXES = ("high", "low")

SIN_TERMS = (1.0, -1.66666652e-01, 8.33326050e-03, -1.98281822e-04, 2.65947294e-06)
COS_TERMS = (9.99999995e-01, -4.99999845e-01, 4.16658692e-02, -1.38745501e-03, 2.37459074e-05)


def horner(terms, z):
    total = terms[-1]
    for term in terms[-2::-1]:
        total = total * z + term
    return total


def cos_sin(turn):
    half = turn * 0.5
    z = half * half
    s = half * horner(SIN_TERMS, z)
    c = horner(COS_TERMS, z)
    return 1.0 - 2.0 * s * s, 2.0 * s * c


def bits_of(count):
    return count.bit_length() - 1


def angle_row(angles, layer, group, lanes):
    return cos_sin(jnp.full((1, lanes), angles[layer, group], jnp.float32))


def turn_matrix(count, c, s, flip):
    up, down = (-s, s) if flip else (s, -s)
    height = min(count, 8)
    row = lax.broadcasted_iota(jnp.int32, (height, count), 0)
    column = lax.broadcasted_iota(jnp.int32, (height, count), 1)

    def sides(bit):
        there = (column & (1 << bit)) != 0
        return jnp.where(there, up, c), jnp.where(there, c, down)

    tile = jnp.ones((height, count), jnp.float32)
    for bit in range(bits_of(height)):
        low, high = sides(bit)
        tile = tile * jnp.where((row & (1 << bit)) != 0, high, low)
    tiles = [tile]
    for bit in range(bits_of(height), bits_of(count)):
        low, high = sides(bit)
        tiles = [x * low for x in tiles] + [x * high for x in tiles]
    return jnp.concatenate(tiles, axis=0) if len(tiles) > 1 else tiles[0]


def split(x):
    top = x.astype(jnp.bfloat16)
    return top, (x - top.astype(jnp.float32)).astype(jnp.bfloat16)


def butterflies(values, tangents):
    for bit, tangent in enumerate(tangents):
        new = list(values)
        for i in range(len(values)):
            j = i | (1 << bit)
            if i != j:
                new[i] = values[i] - tangent * values[j]
                new[j] = values[j] + tangent * values[i]
        values = new
    return values


def power(c, n):
    total = c
    for _ in range(n - 1):
        total = total * c
    return total


def mix_rows(parts, matrix):
    high, low = matrix
    left = jnp.concatenate([high, low, high], axis=1)
    highs, lows = zip(*[split(x) for x in parts])
    high, low = jnp.concatenate(highs, axis=1), jnp.concatenate(lows, axis=1)
    return jnp.dot(left, jnp.concatenate([high, high, low], axis=0), preferred_element_type=jnp.float32)


def mix_lanes(x, matrix):
    high, low = matrix
    top, rest = split(x)
    left = jnp.concatenate([top, top, rest], axis=1)
    return jnp.dot(left, jnp.concatenate([high, low, high], axis=0), preferred_element_type=jnp.float32)


def first_kernel(wave_there, levels_there, phases_there, angles_there, out, wave, phases, angles, work, small, large):
    _, blocks, rows, lanes = wave.shape
    chunk = out.shape[2]
    per = rows // chunk

    def level_copy(t):
        part = pl.ds(per * t, per)
        return pltpu.make_async_copy(levels_there.at[part], out.at[part, 2], large.at[0, t])

    def state_copy(t):
        return pltpu.make_async_copy(wave_there.at[:, t], wave.at[:, t], large.at[1, t])

    pltpu.make_async_copy(angles_there, angles, small.at[0]).start()
    pltpu.make_async_copy(phases_there, phases, small.at[1]).start()
    for t in range(blocks):
        level_copy(t).start()
        state_copy(t).start()
    pltpu.make_async_copy(angles_there, angles, small.at[0]).wait()
    c2, s2 = angle_row(angles, 0, 2, lanes)
    scale = power(c2, bits_of(blocks)) if blocks > 1 else jnp.ones_like(c2)
    tangents = [s2 / c2] * bits_of(blocks)
    c1, s1 = angle_row(angles, 0, 1, lanes)
    row_matrix = split(turn_matrix(rows, c1, s1, True))
    c0, s0 = angle_row(angles, 0, 0, lanes)
    lane_matrix = split(turn_matrix(lanes, c0, s0, False))
    pltpu.make_async_copy(phases_there, phases, small.at[1]).wait()
    angle = phases[0:1, :]

    for t in range(blocks):
        level_copy(t).wait()
        state_copy(t).wait()
        c, s = cos_sin(angle * out[per * t : per * (t + 1), 2].reshape(rows, lanes))
        c, s = c * scale, s * scale
        re, im = wave[0, t], wave[1, t]
        both = mix_rows([re * c + im * s, im * c - re * s], row_matrix)
        for p in range(2):
            work[p, t] = both[:, lanes * p : lanes * (p + 1)]
    for p in range(2):
        for k in range(per):
            rows_k = slice(chunk * k, chunk * (k + 1))
            mixed = butterflies([work[p, t, rows_k, :] for t in range(blocks)], tangents)
            for t in range(blocks):
                work[p, t, rows_k, :] = mixed[t]
    for p in range(2):
        for t in range(blocks):
            out[per * t : per * (t + 1), p] = mix_lanes(work[p, t], lane_matrix).reshape(per, chunk, lanes)


def device_kernel(highs, lows, got, phases, angles, out, work):
    count, _, chunk, lanes = got.shape
    low_bits, high_bits = bits_of(lows), bits_of(highs)
    tangents, scale = [], None
    for layer in range(2):
        c2, s2 = angle_row(angles, layer, 2, lanes)
        c3, s3 = angle_row(angles, layer, 3, lanes)
        tangents.append([s3 / c3] * low_bits + [s2 / c2] * high_bits)
        for c in [c3] * low_bits + [c2] * high_bits:
            scale = c if scale is None else scale * c
    angle = phases[1:2, :]

    for first in range(0, chunk, 8):
        rows = slice(first, first + 8)
        for p in range(2):
            mixed = butterflies([got[d, p, rows, :] for d in range(count)], tangents[0])
            for d in range(count):
                work[p, d] = mixed[d]
        for d in range(count):
            c, s = cos_sin(angle * got[d, 2, rows, :])
            c, s = c * scale, s * scale
            re, im = work[0, d], work[1, d]
            work[0, d] = re * c + im * s
            work[1, d] = im * c - re * s
        for p in range(2):
            mixed = butterflies([work[p, d] for d in range(count)], tangents[1])
            for d in range(count):
                out[d, p, rows, :] = mixed[d]


def last_kernel(got, angles, out, keep, send, work, chance):
    _, blocks, rows, lanes = out.shape
    chunk = got.shape[2]
    per = rows // chunk
    pairs, _, part = keep.shape[0], keep.shape[1], keep.shape[2]
    c2, s2 = angle_row(angles, 1, 2, lanes)
    tangents = [s2 / c2] * bits_of(blocks)
    c1, s1 = angle_row(angles, 1, 1, lanes)
    row_matrix = split(turn_matrix(rows, c1, s1, True))
    c0, s0 = angle_row(angles, 1, 0, lanes)
    matrix = turn_matrix(lanes, c0, s0, False)
    if blocks > 1:
        matrix = matrix * power(c2, bits_of(blocks))
    lane_matrix = split(matrix)

    for t in range(blocks):
        both = mix_rows([got[per * t : per * (t + 1), p].reshape(rows, lanes) for p in range(2)], row_matrix)
        for p in range(2):
            work[p, t] = both[:, lanes * p : lanes * (p + 1)]
    for p in range(2):
        for k in range(per):
            rows_k = slice(chunk * k, chunk * (k + 1))
            mixed = butterflies([work[p, t, rows_k, :] for t in range(blocks)], tangents)
            for t in range(blocks):
                work[p, t, rows_k, :] = mixed[t]
    for t in range(blocks):
        re, im = mix_lanes(work[0, t], lane_matrix), mix_lanes(work[1, t], lane_matrix)
        out[0, t] = re
        out[1, t] = im
        sizes = (re * re + im * im).reshape(pairs, 2, part, lanes)
        for side in range(2):
            chance[side, :, t] = sizes[:, side]
    side = lax.rem(lax.axis_index("high"), 2)
    keep[...] = chance[side]
    send[...] = chance[1 - side]


def pair_kernel(keep, got, own, *rest):
    sends, work = rest[:-1], rest[-1]
    work[...] = keep[...] + got[...]
    place = lax.div(lax.axis_index("high"), 2)
    own[...] = work[place]
    for k, send in enumerate(sends):
        send[...] = work[place ^ (k + 1)]


def sum_kernel(scale, *refs):
    total = refs[0][...]
    for ref in refs[1:-1]:
        total = total + ref[...]
    refs[-1][...] = total * scale


VMEM = pl.BlockSpec(memory_space=pltpu.VMEM)
SMEM = pl.BlockSpec(memory_space=pltpu.SMEM)
HBM = pl.BlockSpec(memory_space=pltpu.HBM)


def call(kernel, name, out_shape, in_specs, scratch, args, out_specs=None):
    many = isinstance(out_shape, (list, tuple))
    if out_specs is None:
        out_specs = [VMEM] * len(out_shape) if many else VMEM
    return pl.pallas_call(
        kernel,
        name=name,
        out_shape=out_shape,
        in_specs=in_specs,
        out_specs=out_specs,
        scratch_shapes=scratch,
        compiler_params=pltpu.CompilerParams(vmem_limit_bytes=32 << 20),
    )(*args)


def spread(values):
    return lax.all_to_all(values, AXES, split_axis=0, concat_axis=0, tiled=True)


def shape_of(*extent):
    return jax.ShapeDtypeStruct(extent, jnp.float32)


def with_kernels(wave, levels, phases, angles):
    highs, lows = lax.axis_size("high"), lax.axis_size("low")
    _, blocks, rows, lanes = wave.shape
    count = highs * lows
    chunk = blocks * rows // count
    part = rows // highs
    pairs = highs // 2
    f32 = jnp.float32
    sent = call(
        first_kernel,
        "first",
        shape_of(count, 3, chunk, lanes),
        [HBM] * 4,
        [
            pltpu.VMEM(wave.shape, f32),
            pltpu.VMEM(phases.shape, f32),
            pltpu.SMEM(angles.shape, f32),
            pltpu.VMEM(wave.shape, f32),
            pltpu.SemaphoreType.DMA((2,)),
            pltpu.SemaphoreType.DMA((2, blocks)),
        ],
        tuple(pltpu.with_memory_space_constraint(x, pltpu.HBM) for x in (wave, levels.reshape(count, chunk, lanes), phases, angles)),
    )
    mixed = call(
        functools.partial(device_kernel, highs, lows),
        "device",
        shape_of(count, 2, chunk, lanes),
        [VMEM, VMEM, SMEM],
        [pltpu.VMEM((2, count, 8, lanes), f32)],
        (spread(sent), phases, angles),
    )
    piece = shape_of(pairs, blocks, part, lanes)
    values, keep, send = call(
        last_kernel,
        "last",
        [pltpu.VMEM(wave.shape, f32), piece, piece],
        [VMEM, SMEM],
        [pltpu.VMEM(wave.shape, f32), pltpu.VMEM((2, pairs, blocks, part, lanes), f32)],
        (spread(mixed), angles),
    )
    got = lax.ppermute(send, "high", [(i, i ^ 1) for i in range(highs)])
    own = shape_of(blocks, part, lanes)
    own, *sends = call(pair_kernel, "pair", [own] * pairs, [VMEM, VMEM], [pltpu.VMEM(piece.shape, f32)], (keep, got))
    others = []
    for k in (len(sends) - 1, *range(len(sends) - 1)):
        others.append(lax.ppermute(sends[k], "high", [(i, i ^ (2 * (k + 1))) for i in range(highs)]))
    marginal = call(functools.partial(sum_kernel, 1.0 / highs), "sum", shape_of(blocks, part, lanes), [VMEM] * pairs, [], (own, *others))
    return values, marginal


def apply_along(values, dim, angle):
    count = values.shape[dim]
    table = turn_matrix(count, jnp.cos(angle), jnp.sin(angle), False) if count > 1 else jnp.ones((1, 1), jnp.float32)
    moved = jnp.tensordot(values, table, axes=([dim], [0]), precision=lax.Precision.HIGHEST)
    return jnp.moveaxis(moved, -1, dim)


def phase_step(re, im, levels, angle):
    c, s = cos_sin(angle * levels)
    return re * c + im * s, im * c - re * s


def with_arrays(wave, levels, phases, angles):
    highs, lows = lax.axis_size("high"), lax.axis_size("low")
    _, blocks, rows, lanes = wave.shape
    count = highs * lows
    chunk = blocks * rows // count

    def local(values, layer):
        values = apply_along(values, 3, angles[layer, 0])
        values = apply_along(values, 2, angles[layer, 1])
        return apply_along(values, 1, angles[layer, 2])

    def devices(values, layer):
        values = values.reshape(highs, lows, 2, chunk, lanes)
        values = apply_along(values, 0, angles[layer, 2])
        return apply_along(values, 1, angles[layer, 3]).reshape(count, 2, chunk, lanes)

    values = local(jnp.stack(phase_step(wave[0], wave[1], levels, phases[0])), 0)
    values = jnp.concatenate([values, levels[None]]).reshape(3, count, chunk, lanes).swapaxes(0, 1)
    values = spread(values)
    table = values[:, 2]
    values = devices(values[:, :2], 0)
    values = jnp.stack(phase_step(values[:, 0], values[:, 1], table, phases[1]), axis=1)
    values = spread(devices(values, 1)).swapaxes(0, 1).reshape(wave.shape)
    values = local(values, 1)
    chance = values[0] * values[0] + values[1] * values[1]
    return values, lax.psum_scatter(chance, "high", scatter_dimension=1, tiled=True) / highs


def on_device(wave, levels, phases, angles):
    highs, lows = lax.axis_size("high"), lax.axis_size("low")
    _, blocks, rows, _ = wave.shape
    whole_tiles = blocks * rows % (8 * highs * lows) == 0 and rows % (8 * highs) == 0
    within = rows % max(blocks * rows // (highs * lows), 1) == 0
    if whole_tiles and within and highs % 2 == 0:
        return with_kernels(wave, levels, phases, angles)
    return with_arrays(wave, levels, phases, angles)


def solution(mesh):
    in_specs = (P(None, AXES, None, None), P(AXES, None, None), P(), P())
    out_specs = (P(None, AXES, None, None), P("low", "high", None))
    return jax.shard_map(on_device, mesh=mesh, in_specs=in_specs, out_specs=out_specs, check_vma=False)
```

```python
import functools

import jax
import jax.numpy as jnp
from jax import lax
from jax.experimental import pallas as pl
from jax.experimental.pallas import tpu as pltpu
from jax.sharding import PartitionSpec as P

AXES = ("high", "low")

SIN_TERMS = (1.0, -1.66666652e-01, 8.33326050e-03, -1.98281822e-04, 2.65947294e-06)
COS_TERMS = (9.99999995e-01, -4.99999845e-01, 4.16658692e-02, -1.38745501e-03, 2.37459074e-05)


def horner(terms, z):
    total = terms[-1]
    for term in terms[-2::-1]:
        total = total * z + term
    return total


def cos_sin(turn):
    half = turn * 0.5
    z = half * half
    s = half * horner(SIN_TERMS, z)
    c = horner(COS_TERMS, z)
    return 1.0 - 2.0 * s * s, 2.0 * s * c


def bits_of(count):
    return count.bit_length() - 1


def angle_rows(angles, lanes):
    c, s = cos_sin(angles[...])
    tables = (c, s, s / c)
    return lambda which, layer, group: jnp.broadcast_to(tables[which][layer : layer + 1, group : group + 1], (1, lanes))


def turn_matrix(count, c, s, flip):
    up, down = (-s, s) if flip else (s, -s)
    height = min(count, 8)
    row = lax.broadcasted_iota(jnp.int32, (height, count), 0)
    column = lax.broadcasted_iota(jnp.int32, (height, count), 1)

    def sides(bit):
        there = (column & (1 << bit)) != 0
        return jnp.where(there, up, c), jnp.where(there, c, down)

    tile = jnp.ones((height, count), jnp.float32)
    for bit in range(bits_of(height)):
        low, high = sides(bit)
        tile = tile * jnp.where((row & (1 << bit)) != 0, high, low)
    tiles = [tile]
    for bit in range(bits_of(height), bits_of(count)):
        low, high = sides(bit)
        tiles = [x * low for x in tiles] + [x * high for x in tiles]
    return jnp.concatenate(tiles, axis=0) if len(tiles) > 1 else tiles[0]


def split(x):
    top = x.astype(jnp.bfloat16)
    return top, (x - top.astype(jnp.float32)).astype(jnp.bfloat16)


def butterflies(values, tangents):
    for bit, tangent in enumerate(tangents):
        new = list(values)
        for i in range(len(values)):
            j = i | (1 << bit)
            if i != j:
                new[i] = values[i] - tangent * values[j]
                new[j] = values[j] + tangent * values[i]
        values = new
    return values


def power(c, n):
    total = c
    for _ in range(n - 1):
        total = total * c
    return total


def mix_rows(parts, matrix):
    high, low = matrix
    left = jnp.concatenate([high, low, high], axis=1)
    highs, lows = zip(*[split(x) for x in parts])
    high, low = jnp.concatenate(highs, axis=1), jnp.concatenate(lows, axis=1)
    return jnp.dot(left, jnp.concatenate([high, high, low], axis=0), preferred_element_type=jnp.float32)


def mix_lanes(x, matrix):
    high, low = matrix
    top, rest = split(x)
    left = jnp.concatenate([top, top, rest], axis=1)
    return jnp.dot(left, jnp.concatenate([high, low, high], axis=0), preferred_element_type=jnp.float32)


def first_kernel(wave_there, levels_there, phases_there, angles_there, out, wave, phases, angles, work, small, large):
    _, blocks, rows, lanes = wave.shape
    chunk = out.shape[2]
    per = rows // chunk

    def level_copy(t):
        part = pl.ds(per * t, per)
        return pltpu.make_async_copy(levels_there.at[part], out.at[part, 2], large.at[0, t])

    def state_copy(t):
        return pltpu.make_async_copy(wave_there.at[:, t], wave.at[:, t], large.at[1, t])

    pltpu.make_async_copy(angles_there, angles, small.at[0]).start()
    pltpu.make_async_copy(phases_there, phases, small.at[1]).start()
    for t in range(blocks):
        level_copy(t).start()
        state_copy(t).start()
    pltpu.make_async_copy(angles_there, angles, small.at[0]).wait()
    row_of = angle_rows(angles, lanes)
    c2 = row_of(0, 0, 2)
    scale = power(c2, bits_of(blocks)) if blocks > 1 else jnp.ones_like(c2)
    tangents = [row_of(2, 0, 2)] * bits_of(blocks)
    row_matrix = split(turn_matrix(rows, row_of(0, 0, 1), row_of(1, 0, 1), True))
    lane_matrix = split(turn_matrix(lanes, row_of(0, 0, 0), row_of(1, 0, 0), False))
    pltpu.make_async_copy(phases_there, phases, small.at[1]).wait()
    angle = phases[0:1, :]

    for t in range(blocks):
        level_copy(t).wait()
        state_copy(t).wait()
        c, s = cos_sin(angle * out[per * t : per * (t + 1), 2].reshape(rows, lanes))
        c, s = c * scale, s * scale
        re, im = wave[0, t], wave[1, t]
        both = mix_rows([re * c + im * s, im * c - re * s], row_matrix)
        for p in range(2):
            work[p, t] = both[:, lanes * p : lanes * (p + 1)]
    for p in range(2):
        for k in range(per):
            rows_k = slice(chunk * k, chunk * (k + 1))
            mixed = butterflies([work[p, t, rows_k, :] for t in range(blocks)], tangents)
            for t in range(blocks):
                work[p, t, rows_k, :] = mixed[t]
    for p in range(2):
        for t in range(blocks):
            out[per * t : per * (t + 1), p] = mix_lanes(work[p, t], lane_matrix).reshape(per, chunk, lanes)


def device_kernel(highs, lows, got, phases, angles, out, work):
    count, _, chunk, lanes = got.shape
    low_bits, high_bits = bits_of(lows), bits_of(highs)
    row_of = angle_rows(angles, lanes)
    tangents, scale = [], None
    for layer in range(2):
        tangents.append([row_of(2, layer, 3)] * low_bits + [row_of(2, layer, 2)] * high_bits)
        for c in [row_of(0, layer, 3)] * low_bits + [row_of(0, layer, 2)] * high_bits:
            scale = c if scale is None else scale * c
    angle = phases[1:2, :]

    for first in range(0, chunk, 8):
        rows = slice(first, first + 8)
        for p in range(2):
            mixed = butterflies([got[d, p, rows, :] for d in range(count)], tangents[0])
            for d in range(count):
                work[p, d] = mixed[d]
        for d in range(count):
            c, s = cos_sin(angle * got[d, 2, rows, :])
            c, s = c * scale, s * scale
            re, im = work[0, d], work[1, d]
            work[0, d] = re * c + im * s
            work[1, d] = im * c - re * s
        for p in range(2):
            mixed = butterflies([work[p, d] for d in range(count)], tangents[1])
            for d in range(count):
                out[d, p, rows, :] = mixed[d]


def last_kernel(got, angles, out, keep, send, work, chance):
    _, blocks, rows, lanes = out.shape
    chunk = got.shape[2]
    per = rows // chunk
    pairs, _, part = keep.shape[0], keep.shape[1], keep.shape[2]
    row_of = angle_rows(angles, lanes)
    tangents = [row_of(2, 1, 2)] * bits_of(blocks)
    row_matrix = split(turn_matrix(rows, row_of(0, 1, 1), row_of(1, 1, 1), True))
    matrix = turn_matrix(lanes, row_of(0, 1, 0), row_of(1, 1, 0), False)
    if blocks > 1:
        matrix = matrix * power(row_of(0, 1, 2), bits_of(blocks))
    lane_matrix = split(matrix)

    for t in range(blocks):
        both = mix_rows([got[per * t : per * (t + 1), p].reshape(rows, lanes) for p in range(2)], row_matrix)
        for p in range(2):
            work[p, t] = both[:, lanes * p : lanes * (p + 1)]
    for p in range(2):
        for k in range(per):
            rows_k = slice(chunk * k, chunk * (k + 1))
            mixed = butterflies([work[p, t, rows_k, :] for t in range(blocks)], tangents)
            for t in range(blocks):
                work[p, t, rows_k, :] = mixed[t]
    for t in range(blocks):
        re, im = mix_lanes(work[0, t], lane_matrix), mix_lanes(work[1, t], lane_matrix)
        out[0, t] = re
        out[1, t] = im
        sizes = (re * re + im * im).reshape(pairs, 2, part, lanes)
        for side in range(2):
            chance[side, :, t] = sizes[:, side]
    side = lax.rem(lax.axis_index("high"), 2)
    keep[...] = chance[side]
    send[...] = chance[1 - side]


def pair_kernel(keep, got, own, *rest):
    sends, work = rest[:-1], rest[-1]
    work[...] = keep[...] + got[...]
    place = lax.div(lax.axis_index("high"), 2)
    own[...] = work[place]
    for k, send in enumerate(sends):
        send[...] = work[place ^ (k + 1)]


def sum_kernel(scale, *refs):
    total = refs[0][...]
    for ref in refs[1:-1]:
        total = total + ref[...]
    refs[-1][...] = total * scale


VMEM = pl.BlockSpec(memory_space=pltpu.VMEM)
HBM = pl.BlockSpec(memory_space=pltpu.HBM)


def call(kernel, name, out_shape, in_specs, scratch, args, out_specs=None):
    many = isinstance(out_shape, (list, tuple))
    if out_specs is None:
        out_specs = [VMEM] * len(out_shape) if many else VMEM
    return pl.pallas_call(
        kernel,
        name=name,
        out_shape=out_shape,
        in_specs=in_specs,
        out_specs=out_specs,
        scratch_shapes=scratch,
        compiler_params=pltpu.CompilerParams(vmem_limit_bytes=32 << 20),
    )(*args)


def spread(values):
    return lax.all_to_all(values, AXES, split_axis=0, concat_axis=0, tiled=True)


def shape_of(*extent):
    return jax.ShapeDtypeStruct(extent, jnp.float32)


def with_kernels(wave, levels, phases, angles):
    highs, lows = lax.axis_size("high"), lax.axis_size("low")
    _, blocks, rows, lanes = wave.shape
    count = highs * lows
    chunk = blocks * rows // count
    part = rows // highs
    pairs = highs // 2
    f32 = jnp.float32
    sent = call(
        first_kernel,
        "first",
        shape_of(count, 3, chunk, lanes),
        [HBM] * 4,
        [
            pltpu.VMEM(wave.shape, f32),
            pltpu.VMEM(phases.shape, f32),
            pltpu.VMEM(angles.shape, f32),
            pltpu.VMEM(wave.shape, f32),
            pltpu.SemaphoreType.DMA((2,)),
            pltpu.SemaphoreType.DMA((2, blocks)),
        ],
        tuple(pltpu.with_memory_space_constraint(x, pltpu.HBM) for x in (wave, levels.reshape(count, chunk, lanes), phases, angles)),
    )
    mixed = call(
        functools.partial(device_kernel, highs, lows),
        "device",
        shape_of(count, 2, chunk, lanes),
        [VMEM, VMEM, VMEM],
        [pltpu.VMEM((2, count, 8, lanes), f32)],
        (spread(sent), phases, angles),
    )
    piece = shape_of(pairs, blocks, part, lanes)
    values, keep, send = call(
        last_kernel,
        "last",
        [pltpu.VMEM(wave.shape, f32), piece, piece],
        [VMEM, VMEM],
        [pltpu.VMEM(wave.shape, f32), pltpu.VMEM((2, pairs, blocks, part, lanes), f32)],
        (spread(mixed), angles),
    )
    got = lax.ppermute(send, "high", [(i, i ^ 1) for i in range(highs)])
    own = shape_of(blocks, part, lanes)
    own, *sends = call(pair_kernel, "pair", [own] * pairs, [VMEM, VMEM], [pltpu.VMEM(piece.shape, f32)], (keep, got))
    others = []
    for k in (len(sends) - 1, *range(len(sends) - 1)):
        others.append(lax.ppermute(sends[k], "high", [(i, i ^ (2 * (k + 1))) for i in range(highs)]))
    marginal = call(functools.partial(sum_kernel, 1.0 / highs), "sum", shape_of(blocks, part, lanes), [VMEM] * pairs, [], (own, *others))
    return values, marginal


def apply_along(values, dim, angle):
    count = values.shape[dim]
    table = turn_matrix(count, jnp.cos(angle), jnp.sin(angle), False) if count > 1 else jnp.ones((1, 1), jnp.float32)
    moved = jnp.tensordot(values, table, axes=([dim], [0]), precision=lax.Precision.HIGHEST)
    return jnp.moveaxis(moved, -1, dim)


def phase_step(re, im, levels, angle):
    c, s = cos_sin(angle * levels)
    return re * c + im * s, im * c - re * s


def with_arrays(wave, levels, phases, angles):
    highs, lows = lax.axis_size("high"), lax.axis_size("low")
    _, blocks, rows, lanes = wave.shape
    count = highs * lows
    chunk = blocks * rows // count

    def local(values, layer):
        values = apply_along(values, 3, angles[layer, 0])
        values = apply_along(values, 2, angles[layer, 1])
        return apply_along(values, 1, angles[layer, 2])

    def devices(values, layer):
        values = values.reshape(highs, lows, 2, chunk, lanes)
        values = apply_along(values, 0, angles[layer, 2])
        return apply_along(values, 1, angles[layer, 3]).reshape(count, 2, chunk, lanes)

    values = local(jnp.stack(phase_step(wave[0], wave[1], levels, phases[0])), 0)
    values = jnp.concatenate([values, levels[None]]).reshape(3, count, chunk, lanes).swapaxes(0, 1)
    values = spread(values)
    table = values[:, 2]
    values = devices(values[:, :2], 0)
    values = jnp.stack(phase_step(values[:, 0], values[:, 1], table, phases[1]), axis=1)
    values = spread(devices(values, 1)).swapaxes(0, 1).reshape(wave.shape)
    values = local(values, 1)
    chance = values[0] * values[0] + values[1] * values[1]
    return values, lax.psum_scatter(chance, "high", scatter_dimension=1, tiled=True) / highs


def on_device(wave, levels, phases, angles):
    highs, lows = lax.axis_size("high"), lax.axis_size("low")
    _, blocks, rows, _ = wave.shape
    whole_tiles = blocks * rows % (8 * highs * lows) == 0 and rows % (8 * highs) == 0
    within = rows % max(blocks * rows // (highs * lows), 1) == 0
    if whole_tiles and within and highs % 2 == 0:
        return with_kernels(wave, levels, phases, angles)
    return with_arrays(wave, levels, phases, angles)


def solution(mesh):
    in_specs = (P(None, AXES, None, None), P(AXES, None, None), P(), P())
    out_specs = (P(None, AXES, None, None), P("low", "high", None))
    return jax.shard_map(on_device, mesh=mesh, in_specs=in_specs, out_specs=out_specs, check_vma=False)
```

```python
import functools

import jax
import jax.numpy as jnp
from jax import lax
from jax.experimental import pallas as pl
from jax.experimental.pallas import tpu as pltpu
from jax.sharding import PartitionSpec as P

AXES = ("high", "low")

SIN_TERMS = (1.0, -1.66666652e-01, 8.33326050e-03, -1.98281822e-04, 2.65947294e-06)
COS_TERMS = (9.99999995e-01, -4.99999845e-01, 4.16658692e-02, -1.38745501e-03, 2.37459074e-05)


def horner(terms, z):
    total = terms[-1]
    for term in terms[-2::-1]:
        total = total * z + term
    return total


def cos_sin(turn):
    half = turn * 0.5
    z = half * half
    s = half * horner(SIN_TERMS, z)
    c = horner(COS_TERMS, z)
    return 1.0 - 2.0 * s * s, 2.0 * s * c


def bits_of(count):
    return count.bit_length() - 1


def angle_rows(angles, lanes):
    c, s = cos_sin(angles[...])
    tables = (c, s, s / c)
    return lambda which, layer, group: jnp.broadcast_to(tables[which][layer : layer + 1, group : group + 1], (1, lanes))


def turn_matrix(count, c, s, flip):
    up, down = (-s, s) if flip else (s, -s)
    height = min(count, 8)
    row = lax.broadcasted_iota(jnp.int32, (height, count), 0)
    column = lax.broadcasted_iota(jnp.int32, (height, count), 1)

    def sides(bit):
        there = (column & (1 << bit)) != 0
        return jnp.where(there, up, c), jnp.where(there, c, down)

    tile = jnp.ones((height, count), jnp.float32)
    for bit in range(bits_of(height)):
        low, high = sides(bit)
        tile = tile * jnp.where((row & (1 << bit)) != 0, high, low)
    tiles = [tile]
    for bit in range(bits_of(height), bits_of(count)):
        low, high = sides(bit)
        tiles = [x * low for x in tiles] + [x * high for x in tiles]
    return jnp.concatenate(tiles, axis=0) if len(tiles) > 1 else tiles[0]


def split(x):
    top = x.astype(jnp.bfloat16)
    return top, (x - top.astype(jnp.float32)).astype(jnp.bfloat16)


def butterflies(values, tangents):
    for bit, tangent in enumerate(tangents):
        new = list(values)
        for i in range(len(values)):
            j = i | (1 << bit)
            if i != j:
                new[i] = values[i] - tangent * values[j]
                new[j] = values[j] + tangent * values[i]
        values = new
    return values


def power(c, n):
    total = c
    for _ in range(n - 1):
        total = total * c
    return total


def row_weights(matrix):
    top, rest = split(matrix)
    return jnp.concatenate([jnp.concatenate([top, top], axis=1), jnp.concatenate([rest, jnp.zeros_like(rest)], axis=1)], axis=0)


def lane_weights(matrix):
    top, rest = split(matrix)
    return jnp.concatenate([jnp.concatenate([top, rest], axis=1), jnp.concatenate([top, jnp.zeros_like(rest)], axis=1)], axis=0)


def mix_rows(parts, weights):
    tops, rests = zip(*[split(x) for x in parts])
    right = jnp.concatenate([jnp.concatenate(tops, axis=1), jnp.concatenate(rests, axis=1)], axis=0)
    both = jnp.dot(weights, right, preferred_element_type=jnp.float32)
    rows = both.shape[0] // 2
    return both[:rows] + both[rows:]


def mix_lanes(x, weights):
    both = jnp.dot(jnp.concatenate(split(x), axis=1), weights, preferred_element_type=jnp.float32)
    lanes = x.shape[1]
    return both[:, :lanes] + both[:, lanes:]


def first_kernel(wave_there, levels_there, phases_there, angles_there, out, wave, phases, angles, work, small, large):
    _, blocks, rows, lanes = wave.shape
    chunk = out.shape[2]
    per = rows // chunk

    level_copy = pltpu.make_async_copy(levels_there, out.at[:, 2], large.at[0])
    state_copy = pltpu.make_async_copy(wave_there, wave, large.at[1])

    pltpu.make_async_copy(angles_there, angles, small.at[0]).start()
    pltpu.make_async_copy(phases_there, phases, small.at[1]).start()
    level_copy.start()
    state_copy.start()
    pltpu.make_async_copy(angles_there, angles, small.at[0]).wait()
    row_of = angle_rows(angles, lanes)
    c2 = row_of(0, 0, 2)
    scale = power(c2, bits_of(blocks)) if blocks > 1 else jnp.ones_like(c2)
    tangents = [row_of(2, 0, 2)] * bits_of(blocks)
    row_matrix = row_weights(turn_matrix(rows, row_of(0, 0, 1), row_of(1, 0, 1), True))
    lane_matrix = lane_weights(turn_matrix(lanes, row_of(0, 0, 0), row_of(1, 0, 0), False))
    pltpu.make_async_copy(phases_there, phases, small.at[1]).wait()
    angle = phases[0:1, :]

    level_copy.wait()
    state_copy.wait()
    for t in range(blocks):
        c, s = cos_sin(angle * out[per * t : per * (t + 1), 2].reshape(rows, lanes))
        c, s = c * scale, s * scale
        re, im = wave[0, t], wave[1, t]
        both = mix_rows([re * c + im * s, im * c - re * s], row_matrix)
        for p in range(2):
            work[p, t] = both[:, lanes * p : lanes * (p + 1)]
    for p in range(2):
        for k in range(per):
            rows_k = slice(chunk * k, chunk * (k + 1))
            mixed = butterflies([work[p, t, rows_k, :] for t in range(blocks)], tangents)
            for t in range(blocks):
                work[p, t, rows_k, :] = mixed[t]
    for p in range(2):
        out[:, p] = mix_lanes(work[p].reshape(blocks * rows, lanes), lane_matrix).reshape(blocks * per, chunk, lanes)


def device_kernel(highs, lows, got, phases, angles, out, work):
    count, _, chunk, lanes = got.shape
    low_bits, high_bits = bits_of(lows), bits_of(highs)
    row_of = angle_rows(angles, lanes)
    tangents, scale = [], None
    for layer in range(2):
        tangents.append([row_of(2, layer, 3)] * low_bits + [row_of(2, layer, 2)] * high_bits)
        for c in [row_of(0, layer, 3)] * low_bits + [row_of(0, layer, 2)] * high_bits:
            scale = c if scale is None else scale * c
    angle = phases[1:2, :]

    for first in range(0, chunk, 8):
        rows = slice(first, first + 8)
        for p in range(2):
            mixed = butterflies([got[d, p, rows, :] for d in range(count)], tangents[0])
            for d in range(count):
                work[p, d] = mixed[d]
        for d in range(count):
            c, s = cos_sin(angle * got[d, 2, rows, :])
            c, s = c * scale, s * scale
            re, im = work[0, d], work[1, d]
            work[0, d] = re * c + im * s
            work[1, d] = im * c - re * s
        for p in range(2):
            mixed = butterflies([work[p, d] for d in range(count)], tangents[1])
            for d in range(count):
                out[d, p, rows, :] = mixed[d]


def last_kernel(got, angles, out, keep, send, work, chance):
    _, blocks, rows, lanes = out.shape
    chunk = got.shape[2]
    per = rows // chunk
    pairs, _, part = keep.shape[0], keep.shape[1], keep.shape[2]
    row_of = angle_rows(angles, lanes)
    tangents = [row_of(2, 1, 2)] * bits_of(blocks)
    row_matrix = row_weights(turn_matrix(rows, row_of(0, 1, 1), row_of(1, 1, 1), True))
    matrix = turn_matrix(lanes, row_of(0, 1, 0), row_of(1, 1, 0), False)
    if blocks > 1:
        matrix = matrix * power(row_of(0, 1, 2), bits_of(blocks))
    lane_matrix = lane_weights(matrix)

    for t in range(blocks):
        both = mix_rows([got[per * t : per * (t + 1), p].reshape(rows, lanes) for p in range(2)], row_matrix)
        for p in range(2):
            work[p, t] = both[:, lanes * p : lanes * (p + 1)]
    for p in range(2):
        for k in range(per):
            rows_k = slice(chunk * k, chunk * (k + 1))
            mixed = butterflies([work[p, t, rows_k, :] for t in range(blocks)], tangents)
            for t in range(blocks):
                work[p, t, rows_k, :] = mixed[t]
    for t in range(blocks):
        both = mix_lanes(work[:, t].reshape(2 * rows, lanes), lane_matrix)
        re, im = both[:rows], both[rows:]
        out[0, t] = re
        out[1, t] = im
        sizes = (re * re + im * im).reshape(pairs, 2, part, lanes)
        for side in range(2):
            chance[side, :, t] = sizes[:, side]
    side = lax.rem(lax.axis_index("high"), 2)
    keep[...] = chance[side]
    send[...] = chance[1 - side]


def pair_kernel(keep, got, own, *rest):
    sends, work = rest[:-1], rest[-1]
    work[...] = keep[...] + got[...]
    place = lax.div(lax.axis_index("high"), 2)
    own[...] = work[place]
    for k, send in enumerate(sends):
        send[...] = work[place ^ (k + 1)]


def sum_kernel(scale, *refs):
    total = refs[0][...]
    for ref in refs[1:-1]:
        total = total + ref[...]
    refs[-1][...] = total * scale


VMEM = pl.BlockSpec(memory_space=pltpu.VMEM)
HBM = pl.BlockSpec(memory_space=pltpu.HBM)


def call(kernel, name, out_shape, in_specs, scratch, args, out_specs=None):
    many = isinstance(out_shape, (list, tuple))
    if out_specs is None:
        out_specs = [VMEM] * len(out_shape) if many else VMEM
    return pl.pallas_call(
        kernel,
        name=name,
        out_shape=out_shape,
        in_specs=in_specs,
        out_specs=out_specs,
        scratch_shapes=scratch,
        compiler_params=pltpu.CompilerParams(vmem_limit_bytes=32 << 20),
    )(*args)


def spread(values):
    return lax.all_to_all(values, AXES, split_axis=0, concat_axis=0, tiled=True)


def shape_of(*extent):
    return jax.ShapeDtypeStruct(extent, jnp.float32)


def with_kernels(wave, levels, phases, angles):
    highs, lows = lax.axis_size("high"), lax.axis_size("low")
    _, blocks, rows, lanes = wave.shape
    count = highs * lows
    chunk = blocks * rows // count
    part = rows // highs
    pairs = highs // 2
    f32 = jnp.float32
    sent = call(
        first_kernel,
        "first",
        shape_of(count, 3, chunk, lanes),
        [HBM] * 4,
        [
            pltpu.VMEM(wave.shape, f32),
            pltpu.VMEM(phases.shape, f32),
            pltpu.VMEM(angles.shape, f32),
            pltpu.VMEM(wave.shape, f32),
            pltpu.SemaphoreType.DMA((2,)),
            pltpu.SemaphoreType.DMA((2,)),
        ],
        tuple(pltpu.with_memory_space_constraint(x, pltpu.HBM) for x in (wave, levels.reshape(count, chunk, lanes), phases, angles)),
    )
    mixed = call(
        functools.partial(device_kernel, highs, lows),
        "device",
        shape_of(count, 2, chunk, lanes),
        [VMEM, VMEM, VMEM],
        [pltpu.VMEM((2, count, 8, lanes), f32)],
        (spread(sent), phases, angles),
    )
    piece = shape_of(pairs, blocks, part, lanes)
    values, keep, send = call(
        last_kernel,
        "last",
        [pltpu.VMEM(wave.shape, f32), piece, piece],
        [VMEM, VMEM],
        [pltpu.VMEM(wave.shape, f32), pltpu.VMEM((2, pairs, blocks, part, lanes), f32)],
        (spread(mixed), angles),
    )
    got = lax.ppermute(send, "high", [(i, i ^ 1) for i in range(highs)])
    own = shape_of(blocks, part, lanes)
    own, *sends = call(pair_kernel, "pair", [own] * pairs, [VMEM, VMEM], [pltpu.VMEM(piece.shape, f32)], (keep, got))
    others = []
    for k in (len(sends) - 1, *range(len(sends) - 1)):
        others.append(lax.ppermute(sends[k], "high", [(i, i ^ (2 * (k + 1))) for i in range(highs)]))
    marginal = call(functools.partial(sum_kernel, 1.0 / highs), "sum", shape_of(blocks, part, lanes), [VMEM] * pairs, [], (own, *others))
    return values, marginal


def apply_along(values, dim, angle):
    count = values.shape[dim]
    table = turn_matrix(count, jnp.cos(angle), jnp.sin(angle), False) if count > 1 else jnp.ones((1, 1), jnp.float32)
    moved = jnp.tensordot(values, table, axes=([dim], [0]), precision=lax.Precision.HIGHEST)
    return jnp.moveaxis(moved, -1, dim)


def phase_step(re, im, levels, angle):
    c, s = cos_sin(angle * levels)
    return re * c + im * s, im * c - re * s


def with_arrays(wave, levels, phases, angles):
    highs, lows = lax.axis_size("high"), lax.axis_size("low")
    _, blocks, rows, lanes = wave.shape
    count = highs * lows
    chunk = blocks * rows // count

    def local(values, layer):
        values = apply_along(values, 3, angles[layer, 0])
        values = apply_along(values, 2, angles[layer, 1])
        return apply_along(values, 1, angles[layer, 2])

    def devices(values, layer):
        values = values.reshape(highs, lows, 2, chunk, lanes)
        values = apply_along(values, 0, angles[layer, 2])
        return apply_along(values, 1, angles[layer, 3]).reshape(count, 2, chunk, lanes)

    values = local(jnp.stack(phase_step(wave[0], wave[1], levels, phases[0])), 0)
    values = jnp.concatenate([values, levels[None]]).reshape(3, count, chunk, lanes).swapaxes(0, 1)
    values = spread(values)
    table = values[:, 2]
    values = devices(values[:, :2], 0)
    values = jnp.stack(phase_step(values[:, 0], values[:, 1], table, phases[1]), axis=1)
    values = spread(devices(values, 1)).swapaxes(0, 1).reshape(wave.shape)
    values = local(values, 1)
    chance = values[0] * values[0] + values[1] * values[1]
    return values, lax.psum_scatter(chance, "high", scatter_dimension=1, tiled=True) / highs


def on_device(wave, levels, phases, angles):
    highs, lows = lax.axis_size("high"), lax.axis_size("low")
    _, blocks, rows, _ = wave.shape
    whole_tiles = blocks * rows % (8 * highs * lows) == 0 and rows % (8 * highs) == 0
    within = rows % max(blocks * rows // (highs * lows), 1) == 0
    if whole_tiles and within and highs % 2 == 0:
        return with_kernels(wave, levels, phases, angles)
    return with_arrays(wave, levels, phases, angles)


def solution(mesh):
    in_specs = (P(None, AXES, None, None), P(AXES, None, None), P(), P())
    out_specs = (P(None, AXES, None, None), P("low", "high", None))
    return jax.shard_map(on_device, mesh=mesh, in_specs=in_specs, out_specs=out_specs, check_vma=False)
```

```python
import functools

import jax
import jax.numpy as jnp
from jax import lax
from jax.experimental import pallas as pl
from jax.experimental.pallas import tpu as pltpu
from jax.sharding import PartitionSpec as P

AXES = ("high", "low")

SIN_TERMS = (1.0, -1.66666652e-01, 8.33326050e-03, -1.98281822e-04, 2.65947294e-06)
COS_TERMS = (9.99999995e-01, -4.99999845e-01, 4.16658692e-02, -1.38745501e-03, 2.37459074e-05)


def horner(terms, z):
    total = terms[-1]
    for term in terms[-2::-1]:
        total = total * z + term
    return total


def cos_sin(turn):
    half = turn * 0.5
    z = half * half
    s = half * horner(SIN_TERMS, z)
    c = horner(COS_TERMS, z)
    return 1.0 - 2.0 * s * s, 2.0 * s * c


def bits_of(count):
    return count.bit_length() - 1


def angle_rows(angles, lanes):
    c, s = cos_sin(angles[...])
    tables = (c, s, s / c)
    return lambda which, layer, group: jnp.broadcast_to(tables[which][layer : layer + 1, group : group + 1], (1, lanes))


def turn_matrix(count, c, s, flip):
    up, down = (-s, s) if flip else (s, -s)
    height = min(count, 8)
    row = lax.broadcasted_iota(jnp.int32, (height, count), 0)
    column = lax.broadcasted_iota(jnp.int32, (height, count), 1)

    def sides(bit):
        there = (column & (1 << bit)) != 0
        return jnp.where(there, up, c), jnp.where(there, c, down)

    tile = jnp.ones((height, count), jnp.float32)
    for bit in range(bits_of(height)):
        low, high = sides(bit)
        tile = tile * jnp.where((row & (1 << bit)) != 0, high, low)
    tiles = [tile]
    for bit in range(bits_of(height), bits_of(count)):
        low, high = sides(bit)
        tiles = [x * low for x in tiles] + [x * high for x in tiles]
    return jnp.concatenate(tiles, axis=0) if len(tiles) > 1 else tiles[0]


def split(x):
    top = x.astype(jnp.bfloat16)
    return top, (x - top.astype(jnp.float32)).astype(jnp.bfloat16)


def butterflies(values, tangents):
    for bit, tangent in enumerate(tangents):
        new = list(values)
        for i in range(len(values)):
            j = i | (1 << bit)
            if i != j:
                new[i] = values[i] - tangent * values[j]
                new[j] = values[j] + tangent * values[i]
        values = new
    return values


def power(c, n):
    total = c
    for _ in range(n - 1):
        total = total * c
    return total


def row_weights(matrix):
    top, rest = split(matrix)
    return jnp.concatenate([jnp.concatenate([top, top], axis=1), jnp.concatenate([rest, jnp.zeros_like(rest)], axis=1)], axis=0)


def lane_weights(matrix):
    top, rest = split(matrix)
    return jnp.concatenate([jnp.concatenate([top, rest], axis=1), jnp.concatenate([top, jnp.zeros_like(rest)], axis=1)], axis=0)


def mix_rows(parts, weights):
    tops, rests = zip(*[split(x) for x in parts])
    right = jnp.concatenate([jnp.concatenate(tops, axis=1), jnp.concatenate(rests, axis=1)], axis=0)
    both = jnp.dot(weights, right, preferred_element_type=jnp.float32)
    rows = both.shape[0] // 2
    return both[:rows] + both[rows:]


def mix_lanes(x, weights):
    both = jnp.dot(jnp.concatenate(split(x), axis=1), weights, preferred_element_type=jnp.float32)
    lanes = x.shape[1]
    return both[:, :lanes] + both[:, lanes:]


def first_kernel(wave_there, levels_there, phases_there, angles_there, out, wave, phases, angles, work, small, large):
    _, blocks, rows, lanes = wave.shape
    chunk = out.shape[2]
    per = rows // chunk

    level_copy = pltpu.make_async_copy(levels_there, out.at[:, 2], large.at[0])
    state_copy = pltpu.make_async_copy(wave_there, wave, large.at[1])

    pltpu.make_async_copy(angles_there, angles, small.at[0]).start()
    pltpu.make_async_copy(phases_there, phases, small.at[1]).start()
    level_copy.start()
    state_copy.start()
    pltpu.make_async_copy(angles_there, angles, small.at[0]).wait()
    row_of = angle_rows(angles, lanes)
    c2 = row_of(0, 0, 2)
    scale = power(c2, bits_of(blocks)) if blocks > 1 else jnp.ones_like(c2)
    tangents = [row_of(2, 0, 2)] * bits_of(blocks)
    row_matrix = row_weights(turn_matrix(rows, row_of(0, 0, 1), row_of(1, 0, 1), True))
    lane_matrix = lane_weights(turn_matrix(lanes, row_of(0, 0, 0), row_of(1, 0, 0), False))
    pltpu.make_async_copy(phases_there, phases, small.at[1]).wait()
    angle = phases[0:1, :]

    level_copy.wait()
    for t in range(blocks):
        c, s = cos_sin(angle * out[per * t : per * (t + 1), 2].reshape(rows, lanes))
        work[0, t] = c * scale
        work[1, t] = s * scale
    state_copy.wait()
    for t in range(blocks):
        c, s = work[0, t], work[1, t]
        re, im = wave[0, t], wave[1, t]
        both = mix_rows([re * c + im * s, im * c - re * s], row_matrix)
        for p in range(2):
            work[p, t] = both[:, lanes * p : lanes * (p + 1)]
    for p in range(2):
        for k in range(per):
            rows_k = slice(chunk * k, chunk * (k + 1))
            mixed = butterflies([work[p, t, rows_k, :] for t in range(blocks)], tangents)
            for t in range(blocks):
                work[p, t, rows_k, :] = mixed[t]
    for p in range(2):
        out[:, p] = mix_lanes(work[p].reshape(blocks * rows, lanes), lane_matrix).reshape(blocks * per, chunk, lanes)


def device_kernel(highs, lows, got, phases, angles, out, work):
    count, _, chunk, lanes = got.shape
    low_bits, high_bits = bits_of(lows), bits_of(highs)
    row_of = angle_rows(angles, lanes)
    tangents, scale = [], None
    for layer in range(2):
        tangents.append([row_of(2, layer, 3)] * low_bits + [row_of(2, layer, 2)] * high_bits)
        for c in [row_of(0, layer, 3)] * low_bits + [row_of(0, layer, 2)] * high_bits:
            scale = c if scale is None else scale * c
    angle = phases[1:2, :]

    for first in range(0, chunk, 8):
        rows = slice(first, first + 8)
        for p in range(2):
            mixed = butterflies([got[d, p, rows, :] for d in range(count)], tangents[0])
            for d in range(count):
                work[p, d] = mixed[d]
        for d in range(count):
            c, s = cos_sin(angle * got[d, 2, rows, :])
            c, s = c * scale, s * scale
            re, im = work[0, d], work[1, d]
            work[0, d] = re * c + im * s
            work[1, d] = im * c - re * s
        for p in range(2):
            mixed = butterflies([work[p, d] for d in range(count)], tangents[1])
            for d in range(count):
                out[d, p, rows, :] = mixed[d]


def last_kernel(got, angles, out, keep, send, work, chance):
    _, blocks, rows, lanes = out.shape
    chunk = got.shape[2]
    per = rows // chunk
    pairs, _, part = keep.shape[0], keep.shape[1], keep.shape[2]
    row_of = angle_rows(angles, lanes)
    tangents = [row_of(2, 1, 2)] * bits_of(blocks)
    row_matrix = row_weights(turn_matrix(rows, row_of(0, 1, 1), row_of(1, 1, 1), True))
    matrix = turn_matrix(lanes, row_of(0, 1, 0), row_of(1, 1, 0), False)
    if blocks > 1:
        matrix = matrix * power(row_of(0, 1, 2), bits_of(blocks))
    lane_matrix = lane_weights(matrix)

    for t in range(blocks):
        both = mix_rows([got[per * t : per * (t + 1), p].reshape(rows, lanes) for p in range(2)], row_matrix)
        for p in range(2):
            work[p, t] = both[:, lanes * p : lanes * (p + 1)]
    for p in range(2):
        for k in range(per):
            rows_k = slice(chunk * k, chunk * (k + 1))
            mixed = butterflies([work[p, t, rows_k, :] for t in range(blocks)], tangents)
            for t in range(blocks):
                work[p, t, rows_k, :] = mixed[t]
    for t in range(blocks):
        both = mix_lanes(work[:, t].reshape(2 * rows, lanes), lane_matrix)
        re, im = both[:rows], both[rows:]
        out[0, t] = re
        out[1, t] = im
        sizes = (re * re + im * im).reshape(pairs, 2, part, lanes)
        for side in range(2):
            chance[side, :, t] = sizes[:, side]
    side = lax.rem(lax.axis_index("high"), 2)
    keep[...] = chance[side]
    send[...] = chance[1 - side]


def pair_kernel(keep, got, own, *rest):
    sends, work = rest[:-1], rest[-1]
    work[...] = keep[...] + got[...]
    place = lax.div(lax.axis_index("high"), 2)
    own[...] = work[place]
    for k, send in enumerate(sends):
        send[...] = work[place ^ (k + 1)]


def sum_kernel(scale, *refs):
    total = refs[0][...]
    for ref in refs[1:-1]:
        total = total + ref[...]
    refs[-1][...] = total * scale


VMEM = pl.BlockSpec(memory_space=pltpu.VMEM)
HBM = pl.BlockSpec(memory_space=pltpu.HBM)


def call(kernel, name, out_shape, in_specs, scratch, args, out_specs=None):
    many = isinstance(out_shape, (list, tuple))
    if out_specs is None:
        out_specs = [VMEM] * len(out_shape) if many else VMEM
    return pl.pallas_call(
        kernel,
        name=name,
        out_shape=out_shape,
        in_specs=in_specs,
        out_specs=out_specs,
        scratch_shapes=scratch,
        compiler_params=pltpu.CompilerParams(vmem_limit_bytes=32 << 20),
    )(*args)


def spread(values):
    return lax.all_to_all(values, AXES, split_axis=0, concat_axis=0, tiled=True)


def shape_of(*extent):
    return jax.ShapeDtypeStruct(extent, jnp.float32)


def with_kernels(wave, levels, phases, angles):
    highs, lows = lax.axis_size("high"), lax.axis_size("low")
    _, blocks, rows, lanes = wave.shape
    count = highs * lows
    chunk = blocks * rows // count
    part = rows // highs
    pairs = highs // 2
    f32 = jnp.float32
    sent = call(
        first_kernel,
        "first",
        shape_of(count, 3, chunk, lanes),
        [HBM] * 4,
        [
            pltpu.VMEM(wave.shape, f32),
            pltpu.VMEM(phases.shape, f32),
            pltpu.VMEM(angles.shape, f32),
            pltpu.VMEM(wave.shape, f32),
            pltpu.SemaphoreType.DMA((2,)),
            pltpu.SemaphoreType.DMA((2,)),
        ],
        tuple(pltpu.with_memory_space_constraint(x, pltpu.HBM) for x in (wave, levels.reshape(count, chunk, lanes), phases, angles)),
    )
    mixed = call(
        functools.partial(device_kernel, highs, lows),
        "device",
        shape_of(count, 2, chunk, lanes),
        [VMEM, VMEM, VMEM],
        [pltpu.VMEM((2, count, 8, lanes), f32)],
        (spread(sent), phases, angles),
    )
    piece = shape_of(pairs, blocks, part, lanes)
    values, keep, send = call(
        last_kernel,
        "last",
        [pltpu.VMEM(wave.shape, f32), piece, piece],
        [VMEM, VMEM],
        [pltpu.VMEM(wave.shape, f32), pltpu.VMEM((2, pairs, blocks, part, lanes), f32)],
        (spread(mixed), angles),
    )
    got = lax.ppermute(send, "high", [(i, i ^ 1) for i in range(highs)])
    own = shape_of(blocks, part, lanes)
    own, *sends = call(pair_kernel, "pair", [own] * pairs, [VMEM, VMEM], [pltpu.VMEM(piece.shape, f32)], (keep, got))
    others = []
    for k in (len(sends) - 1, *range(len(sends) - 1)):
        others.append(lax.ppermute(sends[k], "high", [(i, i ^ (2 * (k + 1))) for i in range(highs)]))
    marginal = call(functools.partial(sum_kernel, 1.0 / highs), "sum", shape_of(blocks, part, lanes), [VMEM] * pairs, [], (own, *others))
    return values, marginal


def apply_along(values, dim, angle):
    count = values.shape[dim]
    table = turn_matrix(count, jnp.cos(angle), jnp.sin(angle), False) if count > 1 else jnp.ones((1, 1), jnp.float32)
    moved = jnp.tensordot(values, table, axes=([dim], [0]), precision=lax.Precision.HIGHEST)
    return jnp.moveaxis(moved, -1, dim)


def phase_step(re, im, levels, angle):
    c, s = cos_sin(angle * levels)
    return re * c + im * s, im * c - re * s


def with_arrays(wave, levels, phases, angles):
    highs, lows = lax.axis_size("high"), lax.axis_size("low")
    _, blocks, rows, lanes = wave.shape
    count = highs * lows
    chunk = blocks * rows // count

    def local(values, layer):
        values = apply_along(values, 3, angles[layer, 0])
        values = apply_along(values, 2, angles[layer, 1])
        return apply_along(values, 1, angles[layer, 2])

    def devices(values, layer):
        values = values.reshape(highs, lows, 2, chunk, lanes)
        values = apply_along(values, 0, angles[layer, 2])
        return apply_along(values, 1, angles[layer, 3]).reshape(count, 2, chunk, lanes)

    values = local(jnp.stack(phase_step(wave[0], wave[1], levels, phases[0])), 0)
    values = jnp.concatenate([values, levels[None]]).reshape(3, count, chunk, lanes).swapaxes(0, 1)
    values = spread(values)
    table = values[:, 2]
    values = devices(values[:, :2], 0)
    values = jnp.stack(phase_step(values[:, 0], values[:, 1], table, phases[1]), axis=1)
    values = spread(devices(values, 1)).swapaxes(0, 1).reshape(wave.shape)
    values = local(values, 1)
    chance = values[0] * values[0] + values[1] * values[1]
    return values, lax.psum_scatter(chance, "high", scatter_dimension=1, tiled=True) / highs


def on_device(wave, levels, phases, angles):
    highs, lows = lax.axis_size("high"), lax.axis_size("low")
    _, blocks, rows, _ = wave.shape
    whole_tiles = blocks * rows % (8 * highs * lows) == 0 and rows % (8 * highs) == 0
    within = rows % max(blocks * rows // (highs * lows), 1) == 0
    if whole_tiles and within and highs % 2 == 0:
        return with_kernels(wave, levels, phases, angles)
    return with_arrays(wave, levels, phases, angles)


def solution(mesh):
    in_specs = (P(None, AXES, None, None), P(AXES, None, None), P(), P())
    out_specs = (P(None, AXES, None, None), P("low", "high", None))
    return jax.shard_map(on_device, mesh=mesh, in_specs=in_specs, out_specs=out_specs, check_vma=False)
```

```python
import functools

import jax
import jax.numpy as jnp
from jax import lax
from jax.experimental import pallas as pl
from jax.experimental.pallas import tpu as pltpu
from jax.sharding import Mesh
from jax.sharding import PartitionSpec as P

HIGH, LOW = ("pair", "core"), ("upper", "lower")
AXES = HIGH + LOW
ORDER = ("upper", "lower", "core", "pair")

SIN_TERMS = (1.0, -1.66666652e-01, 8.33326050e-03, -1.98281822e-04, 2.65947294e-06)
COS_TERMS = (9.99999995e-01, -4.99999845e-01, 4.16658692e-02, -1.38745501e-03, 2.37459074e-05)


def horner(terms, z):
    total = terms[-1]
    for term in terms[-2::-1]:
        total = total * z + term
    return total


def cos_sin(turn):
    half = turn * 0.5
    z = half * half
    s = half * horner(SIN_TERMS, z)
    c = horner(COS_TERMS, z)
    return 1.0 - 2.0 * s * s, 2.0 * s * c


def bits_of(count):
    return count.bit_length() - 1


def angle_rows(angles, lanes):
    c, s = cos_sin(angles[...])
    tables = (c, s, s / c)
    return lambda which, layer, group: jnp.broadcast_to(tables[which][layer : layer + 1, group : group + 1], (1, lanes))


def turn_matrix(count, c, s, flip):
    up, down = (-s, s) if flip else (s, -s)
    height = min(count, 8)
    row = lax.broadcasted_iota(jnp.int32, (height, count), 0)
    column = lax.broadcasted_iota(jnp.int32, (height, count), 1)

    def sides(bit):
        there = (column & (1 << bit)) != 0
        return jnp.where(there, up, c), jnp.where(there, c, down)

    tile = jnp.ones((height, count), jnp.float32)
    for bit in range(bits_of(height)):
        low, high = sides(bit)
        tile = tile * jnp.where((row & (1 << bit)) != 0, high, low)
    tiles = [tile]
    for bit in range(bits_of(height), bits_of(count)):
        low, high = sides(bit)
        tiles = [x * low for x in tiles] + [x * high for x in tiles]
    return jnp.concatenate(tiles, axis=0) if len(tiles) > 1 else tiles[0]


def split(x):
    top = x.astype(jnp.bfloat16)
    return top, (x - top.astype(jnp.float32)).astype(jnp.bfloat16)


def butterflies(values, tangents):
    for bit, tangent in enumerate(tangents):
        new = list(values)
        for i in range(len(values)):
            j = i | (1 << bit)
            if i != j:
                new[i] = values[i] - tangent * values[j]
                new[j] = values[j] + tangent * values[i]
        values = new
    return values


def power(c, n):
    total = c
    for _ in range(n - 1):
        total = total * c
    return total


def row_weights(matrix):
    top, rest = split(matrix)
    return jnp.concatenate([jnp.concatenate([top, top], axis=1), jnp.concatenate([rest, jnp.zeros_like(rest)], axis=1)], axis=0)


def lane_weights(matrix):
    top, rest = split(matrix)
    return jnp.concatenate([jnp.concatenate([top, rest], axis=1), jnp.concatenate([top, jnp.zeros_like(rest)], axis=1)], axis=0)


def mix_rows(parts, weights):
    tops, rests = zip(*[split(x) for x in parts])
    right = jnp.concatenate([jnp.concatenate(tops, axis=1), jnp.concatenate(rests, axis=1)], axis=0)
    both = jnp.dot(weights, right, preferred_element_type=jnp.float32)
    rows = both.shape[0] // 2
    return both[:rows] + both[rows:]


def mix_lanes(x, weights):
    both = jnp.dot(jnp.concatenate(split(x), axis=1), weights, preferred_element_type=jnp.float32)
    lanes = x.shape[1]
    return both[:, :lanes] + both[:, lanes:]


def first_kernel(wave_there, levels_there, phases_there, angles_there, out, wave, phases, angles, work, small, large):
    _, blocks, rows, lanes = wave.shape
    chunk = out.shape[2]
    per = rows // chunk

    level_copy = pltpu.make_async_copy(levels_there, out.at[:, 2], large.at[0])
    state_copy = pltpu.make_async_copy(wave_there, wave, large.at[1])

    pltpu.make_async_copy(angles_there, angles, small.at[0]).start()
    pltpu.make_async_copy(phases_there, phases, small.at[1]).start()
    level_copy.start()
    state_copy.start()
    pltpu.make_async_copy(angles_there, angles, small.at[0]).wait()
    row_of = angle_rows(angles, lanes)
    c2 = row_of(0, 0, 2)
    scale = power(c2, bits_of(blocks)) if blocks > 1 else jnp.ones_like(c2)
    tangents = [row_of(2, 0, 2)] * bits_of(blocks)
    row_matrix = row_weights(turn_matrix(rows, row_of(0, 0, 1), row_of(1, 0, 1), True))
    lane_matrix = lane_weights(turn_matrix(lanes, row_of(0, 0, 0), row_of(1, 0, 0), False))
    pltpu.make_async_copy(phases_there, phases, small.at[1]).wait()
    angle = phases[0:1, :]

    level_copy.wait()
    for t in range(blocks):
        c, s = cos_sin(angle * out[per * t : per * (t + 1), 2].reshape(rows, lanes))
        work[0, t] = c * scale
        work[1, t] = s * scale
    state_copy.wait()
    for t in range(blocks):
        c, s = work[0, t], work[1, t]
        re, im = wave[0, t], wave[1, t]
        both = mix_rows([re * c + im * s, im * c - re * s], row_matrix)
        for p in range(2):
            work[p, t] = both[:, lanes * p : lanes * (p + 1)]
    for p in range(2):
        for k in range(per):
            rows_k = slice(chunk * k, chunk * (k + 1))
            mixed = butterflies([work[p, t, rows_k, :] for t in range(blocks)], tangents)
            for t in range(blocks):
                work[p, t, rows_k, :] = mixed[t]
    for p in range(2):
        out[:, p] = mix_lanes(work[p].reshape(blocks * rows, lanes), lane_matrix).reshape(blocks * per, chunk, lanes)


def device_kernel(groups, got, phases, angles, out, work):
    count, _, chunk, lanes = got.shape
    row_of = angle_rows(angles, lanes)
    tangents, scale = [], None
    for layer in range(2):
        tangents.append([row_of(2, layer, group) for group in groups])
        for group in groups:
            c = row_of(0, layer, group)
            scale = c if scale is None else scale * c
    angle = phases[1:2, :]

    for first in range(0, chunk, 8):
        rows = slice(first, first + 8)
        for p in range(2):
            mixed = butterflies([got[d, p, rows, :] for d in range(count)], tangents[0])
            for d in range(count):
                work[p, d] = mixed[d]
        for d in range(count):
            c, s = cos_sin(angle * got[d, 2, rows, :])
            c, s = c * scale, s * scale
            re, im = work[0, d], work[1, d]
            work[0, d] = re * c + im * s
            work[1, d] = im * c - re * s
        for p in range(2):
            mixed = butterflies([work[p, d] for d in range(count)], tangents[1])
            for d in range(count):
                out[d, p, rows, :] = mixed[d]


def last_kernel(got, angles, out, keep, send, work, chance):
    _, blocks, rows, lanes = out.shape
    chunk = got.shape[2]
    per = rows // chunk
    pairs, _, part = keep.shape[0], keep.shape[1], keep.shape[2]
    row_of = angle_rows(angles, lanes)
    tangents = [row_of(2, 1, 2)] * bits_of(blocks)
    row_matrix = row_weights(turn_matrix(rows, row_of(0, 1, 1), row_of(1, 1, 1), True))
    matrix = turn_matrix(lanes, row_of(0, 1, 0), row_of(1, 1, 0), False)
    if blocks > 1:
        matrix = matrix * power(row_of(0, 1, 2), bits_of(blocks))
    lane_matrix = lane_weights(matrix)

    for t in range(blocks):
        both = mix_rows([got[per * t : per * (t + 1), p].reshape(rows, lanes) for p in range(2)], row_matrix)
        for p in range(2):
            work[p, t] = both[:, lanes * p : lanes * (p + 1)]
    for p in range(2):
        for k in range(per):
            rows_k = slice(chunk * k, chunk * (k + 1))
            mixed = butterflies([work[p, t, rows_k, :] for t in range(blocks)], tangents)
            for t in range(blocks):
                work[p, t, rows_k, :] = mixed[t]
    for t in range(blocks):
        both = mix_lanes(work[:, t].reshape(2 * rows, lanes), lane_matrix)
        re, im = both[:rows], both[rows:]
        out[0, t] = re
        out[1, t] = im
        sizes = (re * re + im * im).reshape(pairs, 2, part, lanes)
        for side in range(2):
            chance[side, :, t] = sizes[:, side]
    side = lax.axis_index("core")
    keep[...] = chance[side]
    send[...] = chance[1 - side]


def pair_kernel(keep, got, own, *rest):
    sends, work = rest[:-1], rest[-1]
    work[...] = keep[...] + got[...]
    place = lax.axis_index("pair")
    own[...] = work[place]
    for k, send in enumerate(sends):
        send[...] = work[lax.rem(place + (k + 1), jnp.int32(work.shape[0]))]


def sum_kernel(scale, *refs):
    total = refs[0][...]
    for ref in refs[1:-1]:
        total = total + ref[...]
    refs[-1][...] = total * scale


VMEM = pl.BlockSpec(memory_space=pltpu.VMEM)
HBM = pl.BlockSpec(memory_space=pltpu.HBM)


def call(kernel, name, out_shape, in_specs, scratch, args, out_specs=None):
    many = isinstance(out_shape, (list, tuple))
    if out_specs is None:
        out_specs = [VMEM] * len(out_shape) if many else VMEM
    return pl.pallas_call(
        kernel,
        name=name,
        out_shape=out_shape,
        in_specs=in_specs,
        out_specs=out_specs,
        scratch_shapes=scratch,
        compiler_params=pltpu.CompilerParams(vmem_limit_bytes=32 << 20),
    )(*args)


def groups_of_bits():
    groups = []
    for name in reversed(ORDER):
        groups += [2 if name in HIGH else 3] * bits_of(lax.axis_size(name))
    return groups


def spread(values):
    return lax.all_to_all(values, ORDER, split_axis=0, concat_axis=0, tiled=True)


def shape_of(*extent):
    return jax.ShapeDtypeStruct(extent, jnp.float32)


def with_kernels(wave, levels, phases, angles):
    highs, lows = lax.axis_size(HIGH), lax.axis_size(LOW)
    _, blocks, rows, lanes = wave.shape
    count = highs * lows
    chunk = blocks * rows // count
    part = rows // highs
    pairs = highs // 2
    f32 = jnp.float32
    sent = call(
        first_kernel,
        "first",
        shape_of(count, 3, chunk, lanes),
        [HBM] * 4,
        [
            pltpu.VMEM(wave.shape, f32),
            pltpu.VMEM(phases.shape, f32),
            pltpu.VMEM(angles.shape, f32),
            pltpu.VMEM(wave.shape, f32),
            pltpu.SemaphoreType.DMA((2,)),
            pltpu.SemaphoreType.DMA((2,)),
        ],
        tuple(pltpu.with_memory_space_constraint(x, pltpu.HBM) for x in (wave, levels.reshape(count, chunk, lanes), phases, angles)),
    )
    mixed = call(
        functools.partial(device_kernel, groups_of_bits()),
        "device",
        shape_of(count, 2, chunk, lanes),
        [VMEM, VMEM, VMEM],
        [pltpu.VMEM((2, count, 8, lanes), f32)],
        (spread(sent), phases, angles),
    )
    piece = shape_of(pairs, blocks, part, lanes)
    values, keep, send = call(
        last_kernel,
        "last",
        [pltpu.VMEM(wave.shape, f32), piece, piece],
        [VMEM, VMEM],
        [pltpu.VMEM(wave.shape, f32), pltpu.VMEM((2, pairs, blocks, part, lanes), f32)],
        (spread(mixed), angles),
    )
    got = lax.ppermute(send, HIGH, [(i, i ^ 1) for i in range(highs)])
    own = shape_of(blocks, part, lanes)
    own, *sends = call(pair_kernel, "pair", [own] * pairs, [VMEM, VMEM], [pltpu.VMEM(piece.shape, f32)], (keep, got))
    others = []
    for k in sorted(range(len(sends)), key=lambda k: k != len(sends) // 2):
        others.append(lax.ppermute(sends[k], HIGH, [(i, (i + 2 * (k + 1)) % highs) for i in range(highs)]))
    marginal = call(functools.partial(sum_kernel, 1.0 / highs), "sum", shape_of(blocks, part, lanes), [VMEM] * pairs, [], (own, *others))
    return values, marginal


def apply_along(values, dim, angle):
    count = values.shape[dim]
    table = turn_matrix(count, jnp.cos(angle), jnp.sin(angle), False) if count > 1 else jnp.ones((1, 1), jnp.float32)
    moved = jnp.tensordot(values, table, axes=([dim], [0]), precision=lax.Precision.HIGHEST)
    return jnp.moveaxis(moved, -1, dim)


def phase_step(re, im, levels, angle):
    c, s = cos_sin(angle * levels)
    return re * c + im * s, im * c - re * s


def with_arrays(wave, levels, phases, angles):
    highs, lows = lax.axis_size(HIGH), lax.axis_size(LOW)
    _, blocks, rows, lanes = wave.shape
    count = highs * lows
    chunk = blocks * rows // count

    def local(values, layer):
        values = apply_along(values, 3, angles[layer, 0])
        values = apply_along(values, 2, angles[layer, 1])
        return apply_along(values, 1, angles[layer, 2])

    def devices(values, layer):
        values = values.reshape(*[lax.axis_size(name) for name in ORDER], 2, chunk, lanes)
        for dim, name in enumerate(ORDER):
            values = apply_along(values, dim, angles[layer, 2 if name in HIGH else 3])
        return values.reshape(count, 2, chunk, lanes)

    values = local(jnp.stack(phase_step(wave[0], wave[1], levels, phases[0])), 0)
    values = jnp.concatenate([values, levels[None]]).reshape(3, count, chunk, lanes).swapaxes(0, 1)
    values = spread(values)
    table = values[:, 2]
    values = devices(values[:, :2], 0)
    values = jnp.stack(phase_step(values[:, 0], values[:, 1], table, phases[1]), axis=1)
    values = spread(devices(values, 1)).swapaxes(0, 1).reshape(wave.shape)
    values = local(values, 1)
    chance = values[0] * values[0] + values[1] * values[1]
    return values, lax.psum_scatter(chance, HIGH, scatter_dimension=1, tiled=True) / highs


def on_device(wave, levels, phases, angles):
    highs, lows = lax.axis_size(HIGH), lax.axis_size(LOW)
    _, blocks, rows, _ = wave.shape
    whole_tiles = blocks * rows % (8 * highs * lows) == 0 and rows % (8 * highs) == 0
    within = rows % max(blocks * rows // (highs * lows), 1) == 0
    if whole_tiles and within and highs % 2 == 0:
        return with_kernels(wave, levels, phases, angles)
    return with_arrays(wave, levels, phases, angles)


def solution(mesh):
    highs, lows = mesh.shape["high"], mesh.shape["low"]
    core, lower = 2 - highs % 2, 2 - lows % 2
    fine = Mesh(mesh.devices.reshape(highs // core, core, lows // lower, lower), AXES)
    in_specs = (P(None, AXES, None, None), P(AXES, None, None), P(), P())
    out_specs = (P(None, AXES, None, None), P(LOW, HIGH, None))
    return jax.shard_map(on_device, mesh=fine, in_specs=in_specs, out_specs=out_specs, check_vma=False)
```

```python
import functools

import jax
import jax.numpy as jnp
from jax import lax
from jax.experimental import pallas as pl
from jax.experimental.pallas import tpu as pltpu
from jax.sharding import Mesh
from jax.sharding import PartitionSpec as P

HIGH, LOW = ("far", "near", "core"), ("upper", "lower")
AXES = HIGH + LOW
ORDER = ("upper", "lower", "far", "core", "near")

SIN_TERMS = (1.0, -1.66666652e-01, 8.33326050e-03, -1.98281822e-04, 2.65947294e-06)
COS_TERMS = (9.99999995e-01, -4.99999845e-01, 4.16658692e-02, -1.38745501e-03, 2.37459074e-05)


def horner(terms, z):
    total = terms[-1]
    for term in terms[-2::-1]:
        total = total * z + term
    return total


def cos_sin(turn):
    half = turn * 0.5
    z = half * half
    s = half * horner(SIN_TERMS, z)
    c = horner(COS_TERMS, z)
    return 1.0 - 2.0 * s * s, 2.0 * s * c


def bits_of(count):
    return count.bit_length() - 1


def angle_rows(angles, lanes):
    c, s = cos_sin(angles[...])
    tables = (c, s, s / c)
    return lambda which, layer, group: jnp.broadcast_to(tables[which][layer : layer + 1, group : group + 1], (1, lanes))


def turn_matrix(count, c, s, flip):
    up, down = (-s, s) if flip else (s, -s)
    height = min(count, 8)
    row = lax.broadcasted_iota(jnp.int32, (height, count), 0)
    column = lax.broadcasted_iota(jnp.int32, (height, count), 1)

    def sides(bit):
        there = (column & (1 << bit)) != 0
        return jnp.where(there, up, c), jnp.where(there, c, down)

    tile = jnp.ones((height, count), jnp.float32)
    for bit in range(bits_of(height)):
        low, high = sides(bit)
        tile = tile * jnp.where((row & (1 << bit)) != 0, high, low)
    tiles = [tile]
    for bit in range(bits_of(height), bits_of(count)):
        low, high = sides(bit)
        tiles = [x * low for x in tiles] + [x * high for x in tiles]
    return jnp.concatenate(tiles, axis=0) if len(tiles) > 1 else tiles[0]


def split(x):
    top = x.astype(jnp.bfloat16)
    return top, (x - top.astype(jnp.float32)).astype(jnp.bfloat16)


def butterflies(values, tangents):
    for bit, tangent in enumerate(tangents):
        new = list(values)
        for i in range(len(values)):
            j = i | (1 << bit)
            if i != j:
                new[i] = values[i] - tangent * values[j]
                new[j] = values[j] + tangent * values[i]
        values = new
    return values


def power(c, n):
    total = c
    for _ in range(n - 1):
        total = total * c
    return total


def row_weights(matrix):
    top, rest = split(matrix)
    return jnp.concatenate([jnp.concatenate([top, top], axis=1), jnp.concatenate([rest, jnp.zeros_like(rest)], axis=1)], axis=0)


def lane_weights(matrix):
    top, rest = split(matrix)
    return jnp.concatenate([jnp.concatenate([top, rest], axis=1), jnp.concatenate([top, jnp.zeros_like(rest)], axis=1)], axis=0)


def mix_rows(parts, weights):
    tops, rests = zip(*[split(x) for x in parts])
    right = jnp.concatenate([jnp.concatenate(tops, axis=1), jnp.concatenate(rests, axis=1)], axis=0)
    both = jnp.dot(weights, right, preferred_element_type=jnp.float32)
    rows = both.shape[0] // 2
    return both[:rows] + both[rows:]


def mix_lanes(x, weights):
    both = jnp.dot(jnp.concatenate(split(x), axis=1), weights, preferred_element_type=jnp.float32)
    lanes = x.shape[1]
    return both[:, :lanes] + both[:, lanes:]


def first_kernel(wave_there, levels_there, phases_there, angles_there, out, wave, phases, angles, work, small, large):
    _, blocks, rows, lanes = wave.shape
    chunk = out.shape[2]
    per = rows // chunk

    level_copy = pltpu.make_async_copy(levels_there, out.at[:, 2], large.at[0])
    state_copy = pltpu.make_async_copy(wave_there, wave, large.at[1])

    pltpu.make_async_copy(angles_there, angles, small.at[0]).start()
    pltpu.make_async_copy(phases_there, phases, small.at[1]).start()
    level_copy.start()
    state_copy.start()
    pltpu.make_async_copy(angles_there, angles, small.at[0]).wait()
    row_of = angle_rows(angles, lanes)
    c2 = row_of(0, 0, 2)
    scale = power(c2, bits_of(blocks)) if blocks > 1 else jnp.ones_like(c2)
    tangents = [row_of(2, 0, 2)] * bits_of(blocks)
    row_matrix = row_weights(turn_matrix(rows, row_of(0, 0, 1), row_of(1, 0, 1), True))
    lane_matrix = lane_weights(turn_matrix(lanes, row_of(0, 0, 0), row_of(1, 0, 0), False))
    pltpu.make_async_copy(phases_there, phases, small.at[1]).wait()
    angle = phases[0:1, :]

    level_copy.wait()
    for t in range(blocks):
        c, s = cos_sin(angle * out[per * t : per * (t + 1), 2].reshape(rows, lanes))
        work[0, t] = c * scale
        work[1, t] = s * scale
    state_copy.wait()
    for t in range(blocks):
        c, s = work[0, t], work[1, t]
        re, im = wave[0, t], wave[1, t]
        both = mix_rows([re * c + im * s, im * c - re * s], row_matrix)
        for p in range(2):
            work[p, t] = both[:, lanes * p : lanes * (p + 1)]
    for p in range(2):
        for k in range(per):
            rows_k = slice(chunk * k, chunk * (k + 1))
            mixed = butterflies([work[p, t, rows_k, :] for t in range(blocks)], tangents)
            for t in range(blocks):
                work[p, t, rows_k, :] = mixed[t]
    for p in range(2):
        out[:, p] = mix_lanes(work[p].reshape(blocks * rows, lanes), lane_matrix).reshape(blocks * per, chunk, lanes)


def device_kernel(groups, got, phases, angles, out, work):
    count, _, chunk, lanes = got.shape
    row_of = angle_rows(angles, lanes)
    tangents, scale = [], None
    for layer in range(2):
        tangents.append([row_of(2, layer, group) for group in groups])
        for group in groups:
            c = row_of(0, layer, group)
            scale = c if scale is None else scale * c
    angle = phases[1:2, :]

    for first in range(0, chunk, 8):
        rows = slice(first, first + 8)
        for p in range(2):
            mixed = butterflies([got[d, p, rows, :] for d in range(count)], tangents[0])
            for d in range(count):
                work[p, d] = mixed[d]
        for d in range(count):
            c, s = cos_sin(angle * got[d, 2, rows, :])
            c, s = c * scale, s * scale
            re, im = work[0, d], work[1, d]
            work[0, d] = re * c + im * s
            work[1, d] = im * c - re * s
        for p in range(2):
            mixed = butterflies([work[p, d] for d in range(count)], tangents[1])
            for d in range(count):
                out[d, p, rows, :] = mixed[d]


def last_kernel(got, angles, out, keep, send, work, chance):
    _, blocks, rows, lanes = out.shape
    chunk = got.shape[2]
    per = rows // chunk
    pairs, _, part = keep.shape[0], keep.shape[1], keep.shape[2]
    row_of = angle_rows(angles, lanes)
    tangents = [row_of(2, 1, 2)] * bits_of(blocks)
    row_matrix = row_weights(turn_matrix(rows, row_of(0, 1, 1), row_of(1, 1, 1), True))
    matrix = turn_matrix(lanes, row_of(0, 1, 0), row_of(1, 1, 0), False)
    if blocks > 1:
        matrix = matrix * power(row_of(0, 1, 2), bits_of(blocks))
    lane_matrix = lane_weights(matrix)

    for t in range(blocks):
        both = mix_rows([got[per * t : per * (t + 1), p].reshape(rows, lanes) for p in range(2)], row_matrix)
        for p in range(2):
            work[p, t] = both[:, lanes * p : lanes * (p + 1)]
    for p in range(2):
        for k in range(per):
            rows_k = slice(chunk * k, chunk * (k + 1))
            mixed = butterflies([work[p, t, rows_k, :] for t in range(blocks)], tangents)
            for t in range(blocks):
                work[p, t, rows_k, :] = mixed[t]
    for t in range(blocks):
        both = mix_lanes(work[:, t].reshape(2 * rows, lanes), lane_matrix)
        re, im = both[:rows], both[rows:]
        out[0, t] = re
        out[1, t] = im
        sizes = (re * re + im * im).reshape(pairs, 2, part, lanes)
        for side in range(2):
            chance[side, :, t] = sizes[:, side]
    side = lax.axis_index("core")
    keep[...] = chance[side]
    send[...] = chance[1 - side]


def pair_kernel(keep, got, own, *rest):
    sends, work = rest[:-1], rest[-1]
    work[...] = keep[...] + got[...]
    place = lax.axis_index("far") * lax.axis_size("near") + lax.axis_index("near")
    own[...] = work[place]
    for k, send in enumerate(sends):
        send[...] = work[lax.rem(place + (k + 1), jnp.int32(work.shape[0]))]


def sum_kernel(scale, *refs):
    total = refs[0][...]
    for ref in refs[1:-1]:
        total = total + ref[...]
    refs[-1][...] = total * scale


VMEM = pl.BlockSpec(memory_space=pltpu.VMEM)
HBM = pl.BlockSpec(memory_space=pltpu.HBM)


def call(kernel, name, out_shape, in_specs, scratch, args, out_specs=None):
    many = isinstance(out_shape, (list, tuple))
    if out_specs is None:
        out_specs = [VMEM] * len(out_shape) if many else VMEM
    return pl.pallas_call(
        kernel,
        name=name,
        out_shape=out_shape,
        in_specs=in_specs,
        out_specs=out_specs,
        scratch_shapes=scratch,
        compiler_params=pltpu.CompilerParams(vmem_limit_bytes=32 << 20),
    )(*args)


def groups_of_bits():
    groups = []
    for name in reversed(ORDER):
        groups += [2 if name in HIGH else 3] * bits_of(lax.axis_size(name))
    return groups


def spread(values):
    return lax.all_to_all(values, ORDER, split_axis=0, concat_axis=0, tiled=True)


def shape_of(*extent):
    return jax.ShapeDtypeStruct(extent, jnp.float32)


def with_kernels(wave, levels, phases, angles):
    highs, lows = lax.axis_size(HIGH), lax.axis_size(LOW)
    _, blocks, rows, lanes = wave.shape
    count = highs * lows
    chunk = blocks * rows // count
    part = rows // highs
    pairs = highs // 2
    f32 = jnp.float32
    sent = call(
        first_kernel,
        "first",
        shape_of(count, 3, chunk, lanes),
        [HBM] * 4,
        [
            pltpu.VMEM(wave.shape, f32),
            pltpu.VMEM(phases.shape, f32),
            pltpu.VMEM(angles.shape, f32),
            pltpu.VMEM(wave.shape, f32),
            pltpu.SemaphoreType.DMA((2,)),
            pltpu.SemaphoreType.DMA((2,)),
        ],
        tuple(pltpu.with_memory_space_constraint(x, pltpu.HBM) for x in (wave, levels.reshape(count, chunk, lanes), phases, angles)),
    )
    mixed = call(
        functools.partial(device_kernel, groups_of_bits()),
        "device",
        shape_of(count, 2, chunk, lanes),
        [VMEM, VMEM, VMEM],
        [pltpu.VMEM((2, count, 8, lanes), f32)],
        (spread(sent), phases, angles),
    )
    piece = shape_of(pairs, blocks, part, lanes)
    values, keep, send = call(
        last_kernel,
        "last",
        [pltpu.VMEM(wave.shape, f32), piece, piece],
        [VMEM, VMEM],
        [pltpu.VMEM(wave.shape, f32), pltpu.VMEM((2, pairs, blocks, part, lanes), f32)],
        (spread(mixed), angles),
    )
    got = lax.ppermute(send, HIGH, [(i, i ^ 1) for i in range(highs)])
    own = shape_of(blocks, part, lanes)
    own, *sends = call(pair_kernel, "pair", [own] * pairs, [VMEM, VMEM], [pltpu.VMEM(piece.shape, f32)], (keep, got))
    others = []
    for k in sorted(range(len(sends)), key=lambda k: k != len(sends) // 2):
        others.append(lax.ppermute(sends[k], HIGH, [(i, (i + 2 * (k + 1)) % highs) for i in range(highs)]))
    marginal = call(functools.partial(sum_kernel, 1.0 / highs), "sum", shape_of(blocks, part, lanes), [VMEM] * pairs, [], (own, *others))
    return values, marginal


def apply_along(values, dim, angle):
    count = values.shape[dim]
    table = turn_matrix(count, jnp.cos(angle), jnp.sin(angle), False) if count > 1 else jnp.ones((1, 1), jnp.float32)
    moved = jnp.tensordot(values, table, axes=([dim], [0]), precision=lax.Precision.HIGHEST)
    return jnp.moveaxis(moved, -1, dim)


def phase_step(re, im, levels, angle):
    c, s = cos_sin(angle * levels)
    return re * c + im * s, im * c - re * s


def with_arrays(wave, levels, phases, angles):
    highs, lows = lax.axis_size(HIGH), lax.axis_size(LOW)
    _, blocks, rows, lanes = wave.shape
    count = highs * lows
    chunk = blocks * rows // count

    def local(values, layer):
        values = apply_along(values, 3, angles[layer, 0])
        values = apply_along(values, 2, angles[layer, 1])
        return apply_along(values, 1, angles[layer, 2])

    def devices(values, layer):
        values = values.reshape(*[lax.axis_size(name) for name in ORDER], 2, chunk, lanes)
        for dim, name in enumerate(ORDER):
            values = apply_along(values, dim, angles[layer, 2 if name in HIGH else 3])
        return values.reshape(count, 2, chunk, lanes)

    values = local(jnp.stack(phase_step(wave[0], wave[1], levels, phases[0])), 0)
    values = jnp.concatenate([values, levels[None]]).reshape(3, count, chunk, lanes).swapaxes(0, 1)
    values = spread(values)
    table = values[:, 2]
    values = devices(values[:, :2], 0)
    values = jnp.stack(phase_step(values[:, 0], values[:, 1], table, phases[1]), axis=1)
    values = spread(devices(values, 1)).swapaxes(0, 1).reshape(wave.shape)
    values = local(values, 1)
    chance = values[0] * values[0] + values[1] * values[1]
    return values, lax.psum_scatter(chance, HIGH, scatter_dimension=1, tiled=True) / highs


def on_device(wave, levels, phases, angles):
    highs, lows = lax.axis_size(HIGH), lax.axis_size(LOW)
    _, blocks, rows, _ = wave.shape
    whole_tiles = blocks * rows % (8 * highs * lows) == 0 and rows % (8 * highs) == 0
    within = rows % max(blocks * rows // (highs * lows), 1) == 0
    if whole_tiles and within and highs % 2 == 0:
        return with_kernels(wave, levels, phases, angles)
    return with_arrays(wave, levels, phases, angles)


def solution(mesh):
    highs, lows = mesh.shape["high"], mesh.shape["low"]
    core, lower = 2 - highs % 2, 2 - lows % 2
    far = 2 - highs // core % 2
    fine = Mesh(mesh.devices.reshape(far, highs // core // far, core, lows // lower, lower), AXES)
    in_specs = (P(None, AXES, None, None), P(AXES, None, None), P(), P())
    out_specs = (P(None, AXES, None, None), P(LOW, HIGH, None))
    return jax.shard_map(on_device, mesh=fine, in_specs=in_specs, out_specs=out_specs, check_vma=False)
```

```python
import functools

import jax
import jax.numpy as jnp
from jax import lax
from jax.experimental import pallas as pl
from jax.experimental.pallas import tpu as pltpu
from jax.sharding import Mesh
from jax.sharding import PartitionSpec as P

HIGH, LOW = ("far", "near", "core"), ("upper", "lower")
AXES = HIGH + LOW
ORDER = ("upper", "lower", "far", "core", "near")

SIN_TERMS = (1.0, -1.66666652e-01, 8.33326050e-03, -1.98281822e-04, 2.65947294e-06)
COS_TERMS = (9.99999995e-01, -4.99999845e-01, 4.16658692e-02, -1.38745501e-03, 2.37459074e-05)


def horner(terms, z):
    total = terms[-1]
    for term in terms[-2::-1]:
        total = total * z + term
    return total


def cos_sin(turn):
    return scaled_cos_sin(turn * 0.5, 1.0)


def scaled_cos_sin(half, scale):
    z = half * half
    s = half * horner(SIN_TERMS, z)
    t = s * (2.0 * scale)
    return scale - t * s, t * horner(COS_TERMS, z)


def bits_of(count):
    return count.bit_length() - 1


def angle_rows(angles, lanes):
    c, s = cos_sin(angles[...])
    tables = (c, s, s / c)
    return lambda which, layer, group: jnp.broadcast_to(tables[which][layer : layer + 1, group : group + 1], (1, lanes))


def turn_matrix(count, c, s, flip):
    up, down = (-s, s) if flip else (s, -s)
    height = min(count, 8)
    row = lax.broadcasted_iota(jnp.int32, (height, count), 0)
    column = lax.broadcasted_iota(jnp.int32, (height, count), 1)

    def sides(bit):
        there = (column & (1 << bit)) != 0
        return jnp.where(there, up, c), jnp.where(there, c, down)

    tile = jnp.ones((height, count), jnp.float32)
    for bit in range(bits_of(height)):
        low, high = sides(bit)
        tile = tile * jnp.where((row & (1 << bit)) != 0, high, low)
    tiles = [tile]
    for bit in range(bits_of(height), bits_of(count)):
        low, high = sides(bit)
        tiles = [x * low for x in tiles] + [x * high for x in tiles]
    return jnp.concatenate(tiles, axis=0) if len(tiles) > 1 else tiles[0]


def split(x):
    top = x.astype(jnp.bfloat16)
    return top, (x - top.astype(jnp.float32)).astype(jnp.bfloat16)


def butterflies(values, tangents):
    for bit, tangent in enumerate(tangents):
        new = list(values)
        for i in range(len(values)):
            j = i | (1 << bit)
            if i != j:
                new[i] = values[i] - tangent * values[j]
                new[j] = values[j] + tangent * values[i]
        values = new
    return values


def power(c, n):
    total = c
    for _ in range(n - 1):
        total = total * c
    return total


def row_weights(matrix):
    top, rest = split(matrix)
    return jnp.concatenate([jnp.concatenate([top, top], axis=1), jnp.concatenate([rest, jnp.zeros_like(rest)], axis=1)], axis=0)


def lane_weights(matrix):
    top, rest = split(matrix)
    return jnp.concatenate([jnp.concatenate([top, rest], axis=1), jnp.concatenate([top, jnp.zeros_like(rest)], axis=1)], axis=0)


def mix_rows(parts, weights):
    tops, rests = zip(*[split(x) for x in parts])
    right = jnp.concatenate([jnp.concatenate(tops, axis=1), jnp.concatenate(rests, axis=1)], axis=0)
    both = jnp.dot(weights, right, preferred_element_type=jnp.float32)
    rows = both.shape[0] // 2
    return both[:rows] + both[rows:]


def mix_lanes(x, weights):
    both = jnp.dot(jnp.concatenate(split(x), axis=1), weights, preferred_element_type=jnp.float32)
    lanes = x.shape[1]
    return both[:, :lanes] + both[:, lanes:]


def first_kernel(wave_there, levels_there, phases_there, angles_there, out, wave, phases, angles, work, small, large):
    _, blocks, rows, lanes = wave.shape
    chunk = out.shape[2]
    per = rows // chunk

    level_copy = pltpu.make_async_copy(levels_there, out.at[:, 2], large.at[0])
    state_copy = pltpu.make_async_copy(wave_there, wave, large.at[1])

    pltpu.make_async_copy(angles_there, angles, small.at[0]).start()
    pltpu.make_async_copy(phases_there, phases, small.at[1]).start()
    level_copy.start()
    state_copy.start()
    pltpu.make_async_copy(angles_there, angles, small.at[0]).wait()
    row_of = angle_rows(angles, lanes)
    c2 = row_of(0, 0, 2)
    scale = power(c2, bits_of(blocks)) if blocks > 1 else jnp.ones_like(c2)
    tangents = [row_of(2, 0, 2)] * bits_of(blocks)
    row_matrix = row_weights(turn_matrix(rows, row_of(0, 0, 1), row_of(1, 0, 1), True))
    lane_matrix = lane_weights(turn_matrix(lanes, row_of(0, 0, 0), row_of(1, 0, 0), False))
    pltpu.make_async_copy(phases_there, phases, small.at[1]).wait()
    half_angle = 0.5 * phases[0:1, :]

    level_copy.wait()
    for t in range(blocks):
        c, s = scaled_cos_sin(half_angle * out[per * t : per * (t + 1), 2].reshape(rows, lanes), scale)
        work[0, t] = c
        work[1, t] = s
    state_copy.wait()
    for t in range(blocks):
        c, s = work[0, t], work[1, t]
        re, im = wave[0, t], wave[1, t]
        both = mix_rows([re * c + im * s, im * c - re * s], row_matrix)
        for p in range(2):
            work[p, t] = both[:, lanes * p : lanes * (p + 1)]
    for p in range(2):
        for k in range(per):
            rows_k = slice(chunk * k, chunk * (k + 1))
            mixed = butterflies([work[p, t, rows_k, :] for t in range(blocks)], tangents)
            for t in range(blocks):
                work[p, t, rows_k, :] = mixed[t]
    for p in range(2):
        out[:, p] = mix_lanes(work[p].reshape(blocks * rows, lanes), lane_matrix).reshape(blocks * per, chunk, lanes)


def device_kernel(groups, got, phases, angles, out, work):
    count, _, chunk, lanes = got.shape
    row_of = angle_rows(angles, lanes)
    tangents, scale = [], None
    for layer in range(2):
        tangents.append([row_of(2, layer, group) for group in groups])
        for group in groups:
            c = row_of(0, layer, group)
            scale = c if scale is None else scale * c
    half_angle = 0.5 * phases[1:2, :]

    for first in range(0, chunk, 8):
        rows = slice(first, first + 8)
        for p in range(2):
            mixed = butterflies([got[d, p, rows, :] for d in range(count)], tangents[0])
            for d in range(count):
                work[p, d] = mixed[d]
        for d in range(count):
            c, s = scaled_cos_sin(half_angle * got[d, 2, rows, :], scale)
            re, im = work[0, d], work[1, d]
            work[0, d] = re * c + im * s
            work[1, d] = im * c - re * s
        for p in range(2):
            mixed = butterflies([work[p, d] for d in range(count)], tangents[1])
            for d in range(count):
                out[d, p, rows, :] = mixed[d]


def last_kernel(got, angles, out, keep, send, work, chance):
    _, blocks, rows, lanes = out.shape
    chunk = got.shape[2]
    per = rows // chunk
    pairs, _, part = keep.shape[0], keep.shape[1], keep.shape[2]
    row_of = angle_rows(angles, lanes)
    tangents = [row_of(2, 1, 2)] * bits_of(blocks)
    row_matrix = row_weights(turn_matrix(rows, row_of(0, 1, 1), row_of(1, 1, 1), True))
    matrix = turn_matrix(lanes, row_of(0, 1, 0), row_of(1, 1, 0), False)
    if blocks > 1:
        matrix = matrix * power(row_of(0, 1, 2), bits_of(blocks))
    lane_matrix = lane_weights(matrix)

    for t in range(blocks):
        both = mix_rows([got[per * t : per * (t + 1), p].reshape(rows, lanes) for p in range(2)], row_matrix)
        for p in range(2):
            work[p, t] = both[:, lanes * p : lanes * (p + 1)]
    for p in range(2):
        for k in range(per):
            rows_k = slice(chunk * k, chunk * (k + 1))
            mixed = butterflies([work[p, t, rows_k, :] for t in range(blocks)], tangents)
            for t in range(blocks):
                work[p, t, rows_k, :] = mixed[t]
    for t in range(blocks):
        both = mix_lanes(work[:, t].reshape(2 * rows, lanes), lane_matrix)
        re, im = both[:rows], both[rows:]
        out[0, t] = re
        out[1, t] = im
        sizes = (re * re + im * im).reshape(pairs, 2, part, lanes)
        for side in range(2):
            chance[side, :, t] = sizes[:, side]
    side = lax.axis_index("core")
    keep[...] = chance[side]
    send[...] = chance[1 - side]


def pair_kernel(keep, got, own, *rest):
    sends, work = rest[:-1], rest[-1]
    work[...] = keep[...] + got[...]
    place = lax.axis_index("far") * lax.axis_size("near") + lax.axis_index("near")
    own[...] = work[place]
    for k, send in enumerate(sends):
        send[...] = work[lax.rem(place + (k + 1), jnp.int32(work.shape[0]))]


def sum_kernel(scale, *refs):
    total = refs[0][...]
    for ref in refs[1:-1]:
        total = total + ref[...]
    refs[-1][...] = total * scale


VMEM = pl.BlockSpec(memory_space=pltpu.VMEM)
HBM = pl.BlockSpec(memory_space=pltpu.HBM)


def call(kernel, name, out_shape, in_specs, scratch, args, out_specs=None):
    many = isinstance(out_shape, (list, tuple))
    if out_specs is None:
        out_specs = [VMEM] * len(out_shape) if many else VMEM
    return pl.pallas_call(
        kernel,
        name=name,
        out_shape=out_shape,
        in_specs=in_specs,
        out_specs=out_specs,
        scratch_shapes=scratch,
        compiler_params=pltpu.CompilerParams(vmem_limit_bytes=32 << 20),
    )(*args)


def groups_of_bits():
    groups = []
    for name in reversed(ORDER):
        groups += [2 if name in HIGH else 3] * bits_of(lax.axis_size(name))
    return groups


def spread(values):
    return lax.all_to_all(values, ORDER, split_axis=0, concat_axis=0, tiled=True)


def shape_of(*extent):
    return jax.ShapeDtypeStruct(extent, jnp.float32)


def with_kernels(wave, levels, phases, angles):
    highs, lows = lax.axis_size(HIGH), lax.axis_size(LOW)
    _, blocks, rows, lanes = wave.shape
    count = highs * lows
    chunk = blocks * rows // count
    part = rows // highs
    pairs = highs // 2
    f32 = jnp.float32
    sent = call(
        first_kernel,
        "first",
        shape_of(count, 3, chunk, lanes),
        [HBM] * 4,
        [
            pltpu.VMEM(wave.shape, f32),
            pltpu.VMEM(phases.shape, f32),
            pltpu.VMEM(angles.shape, f32),
            pltpu.VMEM(wave.shape, f32),
            pltpu.SemaphoreType.DMA((2,)),
            pltpu.SemaphoreType.DMA((2,)),
        ],
        tuple(pltpu.with_memory_space_constraint(x, pltpu.HBM) for x in (wave, levels.reshape(count, chunk, lanes), phases, angles)),
    )
    mixed = call(
        functools.partial(device_kernel, groups_of_bits()),
        "device",
        shape_of(count, 2, chunk, lanes),
        [VMEM, VMEM, VMEM],
        [pltpu.VMEM((2, count, 8, lanes), f32)],
        (spread(sent), phases, angles),
    )
    piece = shape_of(pairs, blocks, part, lanes)
    values, keep, send = call(
        last_kernel,
        "last",
        [pltpu.VMEM(wave.shape, f32), piece, piece],
        [VMEM, VMEM],
        [pltpu.VMEM(wave.shape, f32), pltpu.VMEM((2, pairs, blocks, part, lanes), f32)],
        (spread(mixed), angles),
    )
    got = lax.ppermute(send, HIGH, [(i, i ^ 1) for i in range(highs)])
    own = shape_of(blocks, part, lanes)
    own, *sends = call(pair_kernel, "pair", [own] * pairs, [VMEM, VMEM], [pltpu.VMEM(piece.shape, f32)], (keep, got))
    others = []
    for k in sorted(range(len(sends)), key=lambda k: k != len(sends) // 2):
        others.append(lax.ppermute(sends[k], HIGH, [(i, (i + 2 * (k + 1)) % highs) for i in range(highs)]))
    marginal = call(functools.partial(sum_kernel, 1.0 / highs), "sum", shape_of(blocks, part, lanes), [VMEM] * pairs, [], (own, *others))
    return values, marginal


def apply_along(values, dim, angle):
    count = values.shape[dim]
    table = turn_matrix(count, jnp.cos(angle), jnp.sin(angle), False) if count > 1 else jnp.ones((1, 1), jnp.float32)
    moved = jnp.tensordot(values, table, axes=([dim], [0]), precision=lax.Precision.HIGHEST)
    return jnp.moveaxis(moved, -1, dim)


def phase_step(re, im, levels, angle):
    c, s = cos_sin(angle * levels)
    return re * c + im * s, im * c - re * s


def with_arrays(wave, levels, phases, angles):
    highs, lows = lax.axis_size(HIGH), lax.axis_size(LOW)
    _, blocks, rows, lanes = wave.shape
    count = highs * lows
    chunk = blocks * rows // count

    def local(values, layer):
        values = apply_along(values, 3, angles[layer, 0])
        values = apply_along(values, 2, angles[layer, 1])
        return apply_along(values, 1, angles[layer, 2])

    def devices(values, layer):
        values = values.reshape(*[lax.axis_size(name) for name in ORDER], 2, chunk, lanes)
        for dim, name in enumerate(ORDER):
            values = apply_along(values, dim, angles[layer, 2 if name in HIGH else 3])
        return values.reshape(count, 2, chunk, lanes)

    values = local(jnp.stack(phase_step(wave[0], wave[1], levels, phases[0])), 0)
    values = jnp.concatenate([values, levels[None]]).reshape(3, count, chunk, lanes).swapaxes(0, 1)
    values = spread(values)
    table = values[:, 2]
    values = devices(values[:, :2], 0)
    values = jnp.stack(phase_step(values[:, 0], values[:, 1], table, phases[1]), axis=1)
    values = spread(devices(values, 1)).swapaxes(0, 1).reshape(wave.shape)
    values = local(values, 1)
    chance = values[0] * values[0] + values[1] * values[1]
    return values, lax.psum_scatter(chance, HIGH, scatter_dimension=1, tiled=True) / highs


def on_device(wave, levels, phases, angles):
    highs, lows = lax.axis_size(HIGH), lax.axis_size(LOW)
    _, blocks, rows, _ = wave.shape
    whole_tiles = blocks * rows % (8 * highs * lows) == 0 and rows % (8 * highs) == 0
    within = rows % max(blocks * rows // (highs * lows), 1) == 0
    if whole_tiles and within and highs % 2 == 0:
        return with_kernels(wave, levels, phases, angles)
    return with_arrays(wave, levels, phases, angles)


def solution(mesh):
    highs, lows = mesh.shape["high"], mesh.shape["low"]
    core, lower = 2 - highs % 2, 2 - lows % 2
    far = 2 - highs // core % 2
    fine = Mesh(mesh.devices.reshape(far, highs // core // far, core, lows // lower, lower), AXES)
    in_specs = (P(None, AXES, None, None), P(AXES, None, None), P(), P())
    out_specs = (P(None, AXES, None, None), P(LOW, HIGH, None))
    return jax.shard_map(on_device, mesh=fine, in_specs=in_specs, out_specs=out_specs, check_vma=False)
```
